256 devices in a mesh: mode: 64 (over z, y, x_hi), elem: 4 (over x_lo, core).
Axes of the slice: x: 4 (x_hi: 2, x_lo: 2; x = x_hi * 2 + x_lo), y: 4, z: 8, core: 2. Of those that a mesh axis runs over, the one named last changes fastest.
Arguments:
- velocity: float32 [3, 256, 4, 7, 7, 512], P(None, 'mode', None, None, None, 'elem'), may hold values from -0.3 to 0.3
- radial_dx: float32 [4, 7, 7, 512], P(None, None, None, 'elem'), may hold values from 0.5 to 2
- radial_dy: float32 [4, 7, 7, 512], P(None, None, None, 'elem'), may hold values from -0.5 to 0.5
- around_dx: float32 [4, 7, 7, 512], P(None, None, None, 'elem'), may hold values from -0.5 to 0.5
- around_dy: float32 [4, 7, 7, 512], P(None, None, None, 'elem'), may hold values from 0.5 to 2
- jacobian: float32 [4, 7, 7, 512], P(None, None, None, 'elem'), may hold values from 0.5 to 2
Outputs:
- advection: float32 [3, 256, 4, 7, 7, 512], P(None, 'mode', None, None, None, 'elem')
- pressure: float32 [256, 4, 7, 7, 512], P('mode', None, None, None, 'elem')
The draws below stay inside these ranges and needn't reach their ends.
All inputs are finite; a program needn't handle non-finite values.
Results may differ from the reference program's by a relative error of at most 0.0003.
Values sent between devices are 32-bit elements; how exact they have to be, the bound alone decides.
A program may use at most 192 MiB of HBM per device.

```python
import math
import jax
import jax.numpy as jnp
import numpy as np
from jax import lax

PLANES = 256
NODES = 7
ER = 4
ITERS = 3
ET = 512


def level_of(stream_key, dims, cuts, low, largest):
    def one(position, blocks):
        heights = jax.random.uniform(jax.random.fold_in(jax.random.fold_in(stream_key, 6), position), (blocks,), jnp.float32, low / len(cuts), largest / len(cuts))
        return jnp.repeat(jnp.exp(heights), dims[position] // blocks).reshape((-1,) + (1,) * (len(dims) - position - 1))

    factor_of = one(*cuts[0])
    for cut in cuts[1:]:
        factor_of = factor_of * one(*cut)
    return factor_of


def bell_draw(stream_key, shape, spread, bound, shards=(), kind=jnp.bfloat16):
    gain = level_of(stream_key, shape, shards, -0.22, 0.18) if shards else 1.0
    values = jax.random.normal(stream_key, shape, jnp.float32) * spread * gain
    return jnp.minimum(jnp.maximum(values, -bound), bound).astype(kind)


def setup_inputs(seed: int = 0) -> dict:
    keys = jax.random.split(jax.random.key(seed), 7)
    velocity = bell_draw(keys[0], (3, PLANES, ER, NODES, NODES, ET), 0.05, 0.3, ((1, 64), (5, 4)), jnp.float32)
    radial_dx = jnp.clip(jnp.exp(math.log(2.0) - 1.3862944 * jax.random.uniform(keys[1], (ER, NODES, NODES, ET), jnp.float32) ** level_of(keys[1], (ER, NODES, NODES, ET), ((3, 4),), -0.2, 0.2)), 0.5, 2.0)
    radial_dy = jnp.clip(jax.random.uniform(keys[2], (ER, NODES, NODES, ET), jnp.float32, -0.5, 0.5) * level_of(keys[2], (ER, NODES, NODES, ET), ((3, 4),), -0.4, 0.0), -0.5, 0.5)
    around_dx = jnp.clip(jax.random.uniform(keys[3], (ER, NODES, NODES, ET), jnp.float32, -0.5, 0.5) * level_of(keys[3], (ER, NODES, NODES, ET), ((3, 4),), -0.4, 0.0), -0.5, 0.5)
    around_dy = jnp.clip(jnp.exp(math.log(2.0) - 1.3862944 * jax.random.uniform(keys[4], (ER, NODES, NODES, ET), jnp.float32) ** level_of(keys[4], (ER, NODES, NODES, ET), ((3, 4),), -0.2, 0.2)), 0.5, 2.0)
    jacobian = jnp.clip(jnp.exp(math.log(2.0) - 1.3862944 * jax.random.uniform(keys[5], (ER, NODES, NODES, ET), jnp.float32) ** level_of(keys[5], (ER, NODES, NODES, ET), ((3, 4),), -0.2, 0.2)), 0.5, 2.0)
    return dict(velocity=velocity, radial_dx=radial_dx, radial_dy=radial_dy, around_dx=around_dx, around_dy=around_dy, jacobian=jacobian)


spanwise_wave = 2.0 * math.pi / 64.0
time_step = 0.1


def lobatto_rule(count):
    degree = count - 1
    points = np.cos(np.pi * np.arange(count) / degree)
    legendre = np.zeros((count, count))
    for sweep in range(60):
        legendre[:, 0] = 1.0
        legendre[:, 1] = points
        for order in range(2, count):
            legendre[:, order] = ((2 * order - 1) * points * legendre[:, order - 1] - (order - 1) * legendre[:, order - 2]) / order
        points = points - (points * legendre[:, degree] - legendre[:, degree - 1]) / (count * legendre[:, degree])
    legendre[:, 0] = 1.0
    legendre[:, 1] = points
    for order in range(2, count):
        legendre[:, order] = ((2 * order - 1) * points * legendre[:, order - 1] - (order - 1) * legendre[:, order - 2]) / order
    weights = 2.0 / (degree * count * legendre[:, degree] ** 2)
    return points[::-1].copy(), weights[::-1].copy()


def derivative_table():
    lobatto_nodes = lobatto_rule(NODES)[0]
    total = lobatto_nodes.shape[0]
    scales = np.ones(total)
    for column in range(total):
        for other in range(total):
            if other != column:
                scales[column] = scales[column] / (lobatto_nodes[column] - lobatto_nodes[other])
    table = np.zeros((total, total))
    for row in range(total):
        for column in range(total):
            if row != column:
                table[row, column] = scales[column] / scales[row] / (lobatto_nodes[row] - lobatto_nodes[column])
        table[row, row] = -np.sum(table[row])
    return table


def radial_derivative(table, field):
    return jnp.einsum('ia,...abe->...ibe', table, field, precision=lax.Precision.HIGHEST)


def around_derivative(table, field):
    return jnp.einsum('jb,...abe->...aje', table, field, precision=lax.Precision.HIGHEST)


def radial_transpose(table, field):
    return jnp.einsum('ia,...ibe->...abe', table, field, precision=lax.Precision.HIGHEST)


def around_transpose(table, field):
    return jnp.einsum('jb,...aje->...abe', table, field, precision=lax.Precision.HIGHEST)


def z_derivative(field, first_pair):
    shape = field.shape
    count = shape[1] // 2
    pairs = field.reshape((shape[0], count, 2) + shape[2:])
    waves = (first_pair + jnp.arange(count, dtype=jnp.int32)).astype(jnp.float32) * spanwise_wave
    waves = waves.reshape((1, count) + (1,) * (len(shape) - 2))
    return jnp.stack([waves * pairs[:, :, 1], -waves * pairs[:, :, 0]], axis=2).reshape(shape)


def to_physical(spec):
    planes = spec.shape[1]
    inner_part = (spec[:, 2::2] - 1j * spec[:, 3::2]) * (0.5 * planes)
    spectrum = jnp.concatenate([spec[:, 0:1] * planes + 0j, inner_part, spec[:, 1:2] * planes + 0j], axis=1)
    return jnp.fft.irfft(spectrum, n=planes, axis=1).astype(spec.dtype)


def to_spectral(values):
    planes = values.shape[1]
    half = planes // 2
    spectrum = jnp.fft.rfft(values, axis=1)
    mean = jnp.real(spectrum[:, 0:1]) / planes
    top = jnp.real(spectrum[:, half:half + 1]) / planes
    cosine = jnp.real(spectrum[:, 1:half]) * (2.0 / planes)
    sine = -jnp.imag(spectrum[:, 1:half]) * (2.0 / planes)
    pairs = jnp.stack([cosine, sine], axis=2).reshape((values.shape[0], planes - 2) + values.shape[2:])
    return jnp.concatenate([mean, top, pairs], axis=1).astype(values.dtype)


def geometry(radial_dx, radial_dy, around_dx, around_dy, jacobian):
    lobatto_weights = lobatto_rule(NODES)[1]
    quadrature = jnp.asarray(np.outer(lobatto_weights, lobatto_weights), jnp.float32)[:, :, None]
    mass = quadrature * jacobian
    radial_stiff = mass * (radial_dx * radial_dx + radial_dy * radial_dy)
    cross_stiff = mass * (radial_dx * around_dx + radial_dy * around_dy)
    around_stiff = mass * (around_dx * around_dx + around_dy * around_dy)
    return radial_stiff, cross_stiff, around_stiff, mass


def node_weights(layers):
    layer = jnp.arange(layers, dtype=jnp.int32).reshape(layers, 1, 1, 1)
    node = jnp.arange(NODES, dtype=jnp.int32)
    radial_node = node.reshape(1, NODES, 1, 1)
    around_node = node.reshape(1, 1, NODES, 1)
    shared_radial = ((radial_node == NODES - 1) & (layer < layers - 1)) | ((radial_node == 0) & (layer > 0))
    shared_around = (around_node == 0) | (around_node == NODES - 1)
    multiplicity = (1.0 + shared_radial.astype(jnp.float32)) * (1.0 + shared_around.astype(jnp.float32))
    boundary = (radial_node == NODES - 1) & (layer == layers - 1)
    mask = 1.0 - boundary.astype(jnp.float32)
    return mask, mask / multiplicity


def plane_shift(first_plane, count, planes):
    plane = first_plane + jnp.arange(count, dtype=jnp.int32)
    order = jnp.where(plane == 1, planes // 2, plane // 2)
    wave = order.astype(jnp.float32) * spanwise_wave
    return (wave * wave).reshape(count, 1, 1, 1, 1)


def helmholtz_local(table, field, shift, metrics):
    radial_stiff, cross_stiff, around_stiff, mass = metrics
    radial = radial_derivative(table, field)
    beside_all = around_derivative(table, field)
    return (radial_transpose(table, radial_stiff * radial + cross_stiff * beside_all)
            + around_transpose(table, cross_stiff * radial + around_stiff * beside_all)
            + shift * mass * field)


def assemble(field):
    lower = field[:, :-1, -1] + field[:, 1:, 0]
    field = field.at[:, :-1, -1].set(lower).at[:, 1:, 0].set(lower)
    right = field[:, :, :, -1] + jnp.roll(field[:, :, :, 0], -1, axis=-1)
    return field.at[:, :, :, -1].set(right).at[:, :, :, 0].set(jnp.roll(right, 1, axis=-1))


def inner(first, second, weight):
    return jnp.sum(first * second * weight, axis=(1, 2, 3, 4))


def expand(scalar):
    return scalar.reshape(-1, 1, 1, 1, 1)


def reference(velocity, radial_dx, radial_dy, around_dx, around_dy, jacobian):
    table = jnp.asarray(derivative_table(), jnp.float32)
    width = ET // 16

    def advect_block(start):
        start = start.astype(jnp.int32)
        block = lax.dynamic_slice_in_dim(velocity, start, width, 5)
        metric = [lax.dynamic_slice_in_dim(item, start, width, 3) for item in (radial_dx, radial_dy, around_dx, around_dy)]
        radial = radial_derivative(table, block)
        beside_all = around_derivative(table, block)
        along_x = metric[0] * radial + metric[2] * beside_all
        along_y = metric[1] * radial + metric[3] * beside_all
        along_z = z_derivative(block, 0)
        speed = to_physical(block)
        slope_x = to_physical(along_x)
        slope_y = to_physical(along_y)
        slope_z = to_physical(along_z)
        product = -(speed[0:1] * slope_x + speed[1:2] * slope_y + speed[2:3] * slope_z)
        return to_spectral(product)

    blocks = lax.map(advect_block, jnp.arange(16, dtype=jnp.int32) * width)
    advection = jnp.moveaxis(blocks, 0, 5).reshape(velocity.shape)

    metrics = geometry(radial_dx, radial_dy, around_dx, around_dy, jacobian)
    mask, weight = node_weights(ER)
    group = 16

    def pressure_group(start):
        start = start.astype(jnp.int32)
        predicted = lax.dynamic_slice_in_dim(velocity, start, group, 1) + time_step * lax.dynamic_slice_in_dim(advection, start, group, 1)
        radial = radial_derivative(table, predicted[0:2])
        beside_all = around_derivative(table, predicted[0:2])
        divergence = (radial_dx * radial[0] + around_dx * beside_all[0]) + (radial_dy * radial[1] + around_dy * beside_all[1]) + z_derivative(predicted[2:3], start // 2)[0]
        shift = plane_shift(start, group, PLANES)
        right_side = mask * assemble(-(metrics[3] * divergence) / time_step)
        solution = jnp.zeros_like(right_side)
        residual = right_side
        direction = right_side
        norm_now = inner(residual, residual, weight)
        for turn in range(ITERS):
            image = mask * assemble(helmholtz_local(table, direction, shift, metrics))
            alpha = norm_now / inner(direction, image, weight)
            solution = solution + expand(alpha) * direction
            residual = residual - expand(alpha) * image
            norm_next = inner(residual, residual, weight)
            direction = residual + expand(norm_next / norm_now) * direction
            norm_now = norm_next
        return solution

    groups = lax.map(pressure_group, jnp.arange(PLANES // group, dtype=jnp.int32) * group)
    pressure = groups.reshape((PLANES,) + velocity.shape[2:])
    return advection, pressure
```

```python
import functools
import itertools
import math

import jax
import jax.numpy as jnp
import numpy as np
from jax import lax
from jax.experimental import pallas as pl
from jax.experimental.pallas import tpu as pltpu
from jax.sharding import PartitionSpec as P

MESH = pl.DeviceIdType.MESH
NODES = 7
SQUARE = NODES * NODES
LAYERS = 4
ITERS = 3
COMPONENTS = 3
PLANES = 256
MODES = 64
OWN = PLANES // MODES
ELEMS = 4
LANES = 128
CELLS = COMPONENTS * SQUARE * LAYERS
CHUNKS = -(-CELLS // LANES)
PADDED = CHUNKS * LANES
ROWS = CHUNKS * 8
GROUPS = PADDED // 4

spanwise_wave = 2.0 * math.pi / 64.0
time_step = 0.1

VMEM = pltpu.VMEM
DMA = pltpu.SemaphoreType.DMA


def lobatto_rule(count):
    degree = count - 1
    points = np.cos(np.pi * np.arange(count) / degree)
    legendre = np.zeros((count, count))
    for sweep in range(60):
        legendre[:, 0] = 1.0
        legendre[:, 1] = points
        for order in range(2, count):
            legendre[:, order] = (
                (2 * order - 1) * points * legendre[:, order - 1]
                - (order - 1) * legendre[:, order - 2]
            ) / order
        points = points - (points * legendre[:, degree] - legendre[:, degree - 1]) / (
            count * legendre[:, degree]
        )
    legendre[:, 0] = 1.0
    legendre[:, 1] = points
    for order in range(2, count):
        legendre[:, order] = (
            (2 * order - 1) * points * legendre[:, order - 1] - (order - 1) * legendre[:, order - 2]
        ) / order
    weights = 2.0 / (degree * count * legendre[:, degree] ** 2)
    return (points[::-1].copy(), weights[::-1].copy())


def derivative_table():
    lobatto_nodes = lobatto_rule(NODES)[0]
    total = lobatto_nodes.shape[0]
    scales = np.ones(total)
    for column in range(total):
        for other in range(total):
            if other != column:
                scales[column] = scales[column] / (lobatto_nodes[column] - lobatto_nodes[other])
    table = np.zeros((total, total))
    for row in range(total):
        for column in range(total):
            if row != column:
                table[row, column] = (
                    scales[column] / scales[row] / (lobatto_nodes[row] - lobatto_nodes[column])
                )
        table[row, row] = -np.sum(table[row])
    return table


TABLE = derivative_table().astype(np.float32)
WEIGHTS = lobatto_rule(NODES)[1]


def split(value):
    high = value.astype(jnp.bfloat16)
    return (high, (value - high.astype(jnp.float32)).astype(jnp.bfloat16))


def constant_split(value):
    value = value.astype(np.float32)
    high = value.astype(jnp.bfloat16)
    return (high, (value - high.astype(np.float32)).astype(jnp.bfloat16))


def transform_tables():
    position = np.arange(PLANES)
    plane = np.arange(PLANES)
    order = plane // 2
    angle = 2.0 * np.pi / PLANES * ((position[:, None] * order[None, :]) % PLANES)
    is_sine = (plane % 2 == 1)[None, :]
    is_top = (plane == 1)[None, :]
    parity = np.cos(np.pi * (position % 2))[:, None]
    basis = np.where(is_top, parity, np.where(is_sine, np.sin(angle), np.cos(angle)))
    scaling = np.where(order == 0, 1.0, 2.0) / PLANES
    inverse = (basis * scaling[None, :]).T
    wave = (order * spanwise_wave)[None, :]
    slope = np.where(is_sine, wave * np.cos(angle), -wave * np.sin(angle))
    forward = np.concatenate([basis.T, slope.T], axis=1)
    turned = inverse.reshape(MODES, OWN, PLANES).transpose(1, 0, 2).reshape(PLANES, PLANES)
    return (*constant_split(forward), *constant_split(turned))


def swap_halves(value):
    return pltpu.roll(value, 4, value.ndim - 2)


def halves(first, second):
    lower = lax.broadcasted_iota(jnp.int32, first.shape, first.ndim - 2) < 4
    return (
        jnp.where(lower, first, swap_halves(second)),
        jnp.where(lower, swap_halves(first), second),
    )


def pack_kernel(velocity, out, rows):
    for p in range(OWN):
        for c in range(COMPONENTS):
            start = (c * OWN + p) * SQUARE * LAYERS
            rows[p, pl.ds(c * SQUARE * LAYERS, SQUARE * LAYERS), :] = velocity[
                pl.ds(start, SQUARE * LAYERS), :
            ]
        rows[p, pl.ds(CELLS, PADDED - CELLS), :] = jnp.zeros((PADDED - CELLS, LANES), jnp.float32)
        for k in range(CHUNKS):
            turned = rows[p, pl.ds(k * LANES, LANES), :].T
            for t in range(2):
                out[pl.ds(k * 8 + t * 4 + p, MODES, stride=ROWS), :] = turned[
                    t * MODES : (t + 1) * MODES
                ]


def pack(velocity):
    return pl.pallas_call(
        pack_kernel,
        out_shape=jax.ShapeDtypeStruct((MODES * ROWS, LANES), jnp.float32),
        in_specs=[pl.BlockSpec(memory_space=VMEM)],
        out_specs=pl.BlockSpec(memory_space=VMEM),
        scratch_shapes=[VMEM((OWN, PADDED, LANES), jnp.float32)],
        name="pack",
    )(velocity)


def shifted(me, offset):
    z, y, x = (me // 8, lax.rem(me // 2, 4), lax.rem(me, 2))
    dz, dy, dx = offset
    return lax.rem(z + dz, 8) * 8 + lax.rem(y + dy, 4) * 2 + lax.rem(x + dx, 2)


def exchange_order():
    return [o for o in itertools.product(range(8), range(4), range(2)) if o != (0, 0, 0)]


def exchange_kernel(source, target, own_sem, send_sem, receive_sem):
    me = lax.axis_index("mode")
    barrier = pltpu.get_barrier_semaphore()
    order = exchange_order()
    for offset in order:
        pl.semaphore_signal(
            barrier, inc=1, device_id={"mode": shifted(me, offset)}, device_id_type=MESH
        )
    pl.semaphore_wait(barrier, len(order))
    copies = []
    for index, offset in enumerate(order):
        other = shifted(me, offset)
        copy = pltpu.make_async_remote_copy(
            src_ref=source.at[other],
            dst_ref=target.at[me],
            send_sem=send_sem.at[index],
            recv_sem=receive_sem.at[index],
            device_id={"mode": other},
            device_id_type=MESH,
        )
        copy.start()
        copies.append(copy)
    own = pltpu.make_async_copy(source.at[me], target.at[me], own_sem)
    own.start()
    for copy in copies:
        copy.wait()
    own.wait()


def exchange(value, identity):
    return pl.pallas_call(
        exchange_kernel,
        out_shape=jax.ShapeDtypeStruct((MODES, ROWS, LANES), jnp.float32),
        in_specs=[pl.BlockSpec(memory_space=VMEM)],
        out_specs=pl.BlockSpec(memory_space=VMEM),
        scratch_shapes=[DMA, DMA((MODES,)), DMA((MODES,))],
        compiler_params=pltpu.CompilerParams(collective_id=identity, has_side_effects=True),
        name="exchange%d" % identity,
    )(value)


def three_pass(first, second, dims):
    (a, b), (c, d) = (first, second)
    dot = functools.partial(
        lax.dot_general,
        dimension_numbers=(dims, ((), ())),
        preferred_element_type=jnp.float32,
    )
    return dot(a, c) + (dot(a, d) + dot(b, c))


def advect_kernel(received, metrics, forward_high, forward_low, back_high, back_low, out,
                  planes, values, local, result):
    me = lax.axis_index("mode")
    for k in range(CHUNKS):
        block = received[:, pl.ds(k * 8, 8), :].reshape(MODES // 2, 2, 8, LANES)
        pair = halves(block[:, 0], block[:, 1])
        for t in range(2):
            planes[t, :, pl.ds(k * LANES, LANES)] = pair[t].reshape(PLANES, LANES)
    forward = (forward_high[...], forward_low[...])
    sides = []
    for t in range(2):
        sides.append(three_pass(split(planes[t]), forward, ((0,), (0,))))
    first, second = halves(
        sides[0].reshape(PADDED // 8, 8, 2 * PLANES), sides[1].reshape(PADDED // 8, 8, 2 * PLANES)
    )
    for q in range(PADDED // 8):
        values[2 * q] = first[q]
        values[2 * q + 1] = second[q]
    lane = lax.broadcasted_iota(jnp.int32, (SQUARE, 8, LANES), 2)
    sub = lax.broadcasted_iota(jnp.int32, (SQUARE, 8, LANES), 1)
    chosen = lane == me + jnp.where(sub < 4, 0, MODES)
    for i in range(4):
        picked = jnp.sum(jnp.where(chosen, metrics[i], 0.0), axis=2, keepdims=True)
        local[i] = jnp.broadcast_to(-picked, (SQUARE, 8, LANES))
    zero = jnp.zeros((8, PLANES), jnp.float32)
    for a in range(NODES):
        for b in range(NODES):
            node = a * NODES + b
            mx, my, nx, ny = (jnp.concatenate([local[i, node]] * 2, axis=1) for i in range(4))
            u = values[node, :, :PLANES]
            v = values[SQUARE + node, :, :PLANES]
            w = values[2 * SQUARE + node, :, :PLANES]
            along = u * mx + v * my
            across = u * nx + v * ny
            for c in range(COMPONENTS):
                radial, beside = (zero, zero)
                for i in range(NODES):
                    radial += float(TABLE[a, i]) * values[c * SQUARE + i * NODES + b, :, :PLANES]
                    beside += float(TABLE[b, i]) * values[c * SQUARE + a * NODES + i, :, :PLANES]
                slope = values[c * SQUARE + node, :, PLANES:]
                result[c * SQUARE + node] = radial * along + beside * across - slope * w
    for g in range(COMPONENTS * SQUARE, GROUPS):
        result[g] = zero
    paired = result[...].reshape(GROUPS // 2, 2, 8, PLANES)
    sides = halves(paired[:, 0], paired[:, 1])
    back = (back_high[...], back_low[...])
    for t in range(2):
        spectral = three_pass(back, split(sides[t].reshape(PADDED, PLANES)), ((1,), (1,)))
        for p in range(OWN):
            for k in range(CHUNKS):
                out[pl.ds(k * 8 + t * 4 + p, MODES, stride=ROWS), :] = spectral[
                    p * MODES : (p + 1) * MODES, k * LANES : (k + 1) * LANES
                ]


def advect(received, metrics):
    tables = transform_tables()
    return pl.pallas_call(
        advect_kernel,
        out_shape=jax.ShapeDtypeStruct((MODES * ROWS, LANES), jnp.float32),
        in_specs=[pl.BlockSpec(memory_space=VMEM)] * 6,
        out_specs=pl.BlockSpec(memory_space=VMEM),
        scratch_shapes=[
            VMEM((2, PLANES, PADDED), jnp.float32),
            VMEM((GROUPS, 8, 2 * PLANES), jnp.float32),
            VMEM((4, SQUARE, 8, LANES), jnp.float32),
            VMEM((GROUPS, 8, PLANES), jnp.float32),
        ],
        compiler_params=pltpu.CompilerParams(vmem_limit_bytes=40 << 20),
        name="advect",
    )(received, metrics, *(jnp.asarray(t) for t in tables))


def unpack_kernel(returned, velocity, advection, predicted, rows):
    for p in range(OWN):
        for k in range(CHUNKS):
            block = jnp.concatenate(
                [returned[pl.ds(k * 8 + t * 4 + p, MODES, stride=ROWS), :] for t in range(2)],
                axis=0,
            )
            rows[p, pl.ds(k * LANES, LANES), :] = block.T
        for c in range(COMPONENTS):
            start = (c * OWN + p) * SQUARE * LAYERS
            own = pl.ds(c * SQUARE * LAYERS, SQUARE * LAYERS)
            there = rows[p, own, :]
            advection[pl.ds(start, SQUARE * LAYERS), :] = there
            rows[p, own, :] = velocity[pl.ds(start, SQUARE * LAYERS), :] + time_step * there
    for pair in range(OWN // 2):
        first, second = halves(
            rows[2 * pair].reshape(PADDED // 8, 8, LANES),
            rows[2 * pair + 1].reshape(PADDED // 8, 8, LANES),
        )
        for q in range(PADDED // 8):
            predicted[pair, 2 * q] = first[q]
            predicted[pair, 2 * q + 1] = second[q]


def unpack(returned, velocity):
    return pl.pallas_call(
        unpack_kernel,
        out_shape=(
            jax.ShapeDtypeStruct(velocity.shape, jnp.float32),
            jax.ShapeDtypeStruct((OWN // 2, GROUPS, 8, LANES), jnp.float32),
        ),
        in_specs=[pl.BlockSpec(memory_space=VMEM)] * 2,
        out_specs=(pl.BlockSpec(memory_space=VMEM),) * 2,
        scratch_shapes=[VMEM((OWN, PADDED, LANES), jnp.float32)],
        name="unpack",
    )(returned, velocity)


def contract(matrix, field, axis):
    size = NODES
    if axis == 0:
        return [
            functools.reduce(
                lambda x, y: x + y, [float(matrix[i, j]) * field[j] for j in range(size)]
            )
            for i in range(size)
        ]
    return [
        jnp.stack(
            [
                functools.reduce(
                    lambda x, y: x + y, [float(matrix[i, j]) * slab[j] for j in range(size)]
                )
                for i in range(size)
            ]
        )
        for slab in field
    ]


def pressure_kernel(predicted, metrics, out, stiff, rhs, residual, direction, along, local,
                    radial_s, around_s, rims, posts, send_sem, receive_sem):
    me = lax.axis_index("mode")
    here = lax.axis_index("elem")
    barrier = pltpu.get_barrier_semaphore()
    for step in range(1, ELEMS):
        pl.semaphore_signal(
            barrier, inc=1, device_id={"elem": lax.rem(here + step, ELEMS)}, device_id_type=MESH
        )
    pl.semaphore_wait(barrier, ELEMS - 1)

    sub = lax.broadcasted_iota(jnp.int32, (8, LANES), 0)
    lane = lax.broadcasted_iota(jnp.int32, (8, LANES), 1)
    layer = lax.rem(sub, 4)
    even = sub < 4
    inside = layer < LAYERS - 1
    above = layer > 0
    pairs = range(OWN // 2)
    nodes = range(NODES)

    for a in nodes:
        for b in nodes:
            node = a * NODES + b
            rx, ry, ax, ay, jac = (metrics[i, node] for i in range(5))
            mass = float(np.float32(WEIGHTS[a] * WEIGHTS[b])) * jac
            stiff[0, a, b] = mass * (rx * rx + ry * ry)
            stiff[1, a, b] = mass * (rx * ax + ry * ay)
            stiff[2, a, b] = mass * (ax * ax + ay * ay)
            stiff[3, a, b] = mass

    orders = [(me * (OWN // 2) + pair).astype(jnp.float32) for pair in pairs]
    waves = [jnp.full((8, LANES), order) * spanwise_wave for order in orders]
    tops = [
        jnp.where((jnp.full((8, LANES), order) == 0.0) & (sub >= 4), float(PLANES // 2), order)
        * spanwise_wave
        for order in orders
    ]
    shifts = [top * top for top in tops]

    def radial_of(read, a):
        return functools.reduce(
            lambda x, y: x + y, [float(TABLE[a, i]) * read(i) for i in nodes]
        )

    def around_of(slab):
        return [
            functools.reduce(lambda x, y: x + y, [float(TABLE[b, i]) * slab[i] for i in nodes])
            for b in nodes
        ]

    for pair in pairs:
        wave = jnp.where(even, waves[pair], -waves[pair])
        for a in nodes:
            def component(c, i):
                return predicted[pair, pl.ds(c * SQUARE + i * NODES, NODES)]
            radial = [radial_of(functools.partial(component, c), a) for c in range(2)]
            beside = [around_of(component(c, a)) for c in range(2)]
            third = component(2, a)
            for b in nodes:
                node = a * NODES + b
                rx, ry, ax, ay = (metrics[i, node] for i in range(4))
                divergence = (
                    (rx * radial[0][b] + ax * beside[0][b])
                    + (ry * radial[1][b] + ay * beside[1][b])
                    + wave * swap_halves(third[b])
                )
                local[pair, a, b] = -(stiff[3, a, b] * divergence) / time_step

    def across_layers():
        for pair in pairs:
            low, high = (local[pair, 0], local[pair, NODES - 1])
            other = [pltpu.roll(high[b], 1, 0) for b in nodes]
            this = [pltpu.roll(low[b], 7, 0) for b in nodes]
            for b in nodes:
                local[pair, 0, b] = low[b] + jnp.where(above, other[b], 0.0)
                local[pair, NODES - 1, b] = jnp.where(inside, high[b] + this[b], 0.0)

    def talk(phase, dots):
        first = jnp.zeros((8, LANES), jnp.float32)
        last = jnp.zeros((8, LANES), jnp.float32)
        if phase < ITERS:
            for pair in pairs:
                for a in nodes:
                    slot = pair * NODES + a
                    start = local[pair, a, 0]
                    end = local[pair, a, NODES - 1]
                    first = jnp.where(lane == slot, pltpu.roll(start, slot, 1) if slot else start, first)
                    last = jnp.where(lane == slot, pltpu.roll(end, slot + 1, 1), last)
        for index, dot in enumerate(dots):
            total = jnp.sum(dot, axis=1, keepdims=True)
            first = jnp.where(lane == 2 * 8 + index, total, first)
        posts[phase, 0] = first
        posts[phase, 1] = last
        rims[phase, here, 0] = first
        rims[phase, here, 1] = last
        copies = []
        for step in range(1, ELEMS):
            copy = pltpu.make_async_remote_copy(
                src_ref=posts.at[phase],
                dst_ref=rims.at[phase, here],
                send_sem=send_sem.at[phase, step],
                recv_sem=receive_sem.at[phase, step],
                device_id={"elem": lax.rem(here + step, ELEMS)},
                device_id_type=MESH,
            )
            copy.start()
            copies.append(copy)
        for copy in copies:
            copy.wait()
        total = (rims[phase, 0, 0] + rims[phase, 1, 0]) + (rims[phase, 2, 0] + rims[phase, 3, 0])
        sums = []
        for index in range(len(dots)):
            column = jnp.sum(jnp.where(lane == 2 * 8 + index, total, 0.0), axis=1, keepdims=True)
            column = jnp.broadcast_to(column, (8, LANES))
            lower = jnp.sum(jnp.where(even, column, 0.0), axis=0, keepdims=True)
            upper = jnp.sum(jnp.where(even, 0.0, column), axis=0, keepdims=True)
            sums.append(jnp.where(even, lower, upper))
        right = rims[phase, lax.rem(here + 1, ELEMS), 0]
        left = rims[phase, lax.rem(here + ELEMS - 1, ELEMS), 1]
        return (sums, left, right)

    def across_columns(pair, a, left, right):
        slot = pair * NODES + a
        start = local[pair, a, 0]
        end = local[pair, a, NODES - 1]
        after = jnp.where(
            lane == LANES - 1, pltpu.roll(right, LANES - 1 - slot, 1), pltpu.roll(start, LANES - 1, 1)
        )
        before = jnp.where(
            lane == 0, pltpu.roll(left, (LANES - slot) % LANES, 1) if slot else left, pltpu.roll(end, 1, 1)
        )
        return (start + before, end + after)

    across_layers()
    _, left, right = talk(0, [])
    for pair in pairs:
        for a in nodes:
            start, end = across_columns(pair, a, left, right)
            for b in nodes:
                value = start if b == 0 else end if b == NODES - 1 else local[pair, a, b]
                residual[pair, a, b] = value

    weight_a = [
        jnp.where(above, 0.5, 1.0) if a == 0 else jnp.where(inside, 0.5, 0.0) if a == NODES - 1 else None
        for a in nodes
    ]

    gamma_old = [None, None]
    inner_old = [None, None]
    for turn in range(ITERS):
        dots = []
        for pair in pairs:
            norm = jnp.zeros((8, LANES), jnp.float32)
            for a in nodes:
                slab = residual[pair, a]
                radial = radial_of(lambda i: residual[pair, i], a)
                beside = around_of(slab)
                row = jnp.zeros((8, LANES), jnp.float32)
                for b in nodes:
                    g11, g12, g22 = (stiff[i, a, b] for i in range(3))
                    radial_s[a, b] = g11 * radial[b] + g12 * beside[b]
                    around_s[a, b] = g12 * radial[b] + g22 * beside[b]
                    square = slab[b] * slab[b]
                    row = row + (0.5 * square if b in (0, NODES - 1) else square)
                norm = norm + (row if weight_a[a] is None else row * weight_a[a])
            product = jnp.zeros((8, LANES), jnp.float32)
            for a in nodes:
                spread = functools.reduce(
                    lambda x, y: x + y, [float(TABLE[i, a]) * radial_s[i] for i in nodes]
                )
                slab = around_s[a]
                for b in nodes:
                    beside = functools.reduce(
                        lambda x, y: x + y, [float(TABLE[j, b]) * slab[j] for j in nodes]
                    )
                    here_now = residual[pair, a, b]
                    value = spread[b] + beside + shifts[pair] * stiff[3, a, b] * here_now
                    local[pair, a, b] = value
                    product = product + here_now * value
            dots += [norm, product]
        if turn < ITERS - 1:
            across_layers()
        sums, left, right = talk(turn + 1, dots)
        for pair in pairs:
            gamma, delta = (sums[2 * pair], sums[2 * pair + 1])
            if turn == 0:
                beta, inner = (None, delta)
            else:
                beta = gamma / gamma_old[pair]
                inner = delta - beta * beta * inner_old[pair]
            alpha = gamma / inner
            gamma_old[pair], inner_old[pair] = (gamma, inner)
            for a in nodes:
                if turn < ITERS - 1:
                    start, end = across_columns(pair, a, left, right)
                for b in nodes:
                    now = residual[pair, a, b]
                    if turn:
                        now = now + beta * direction[pair, a, b]
                    step = alpha * now
                    out[pair, a, b] = step if turn == 0 else out[pair, a, b] + step
                    if turn < ITERS - 1:
                        direction[pair, a, b] = now
                        image = start if b == 0 else end if b == NODES - 1 else local[pair, a, b]
                        if turn:
                            image = image + beta * along[pair, a, b]
                        along[pair, a, b] = image
                        residual[pair, a, b] = residual[pair, a, b] - alpha * image


def pressure_of(predicted, metrics):
    field = VMEM((OWN // 2, NODES, NODES, 8, LANES), jnp.float32)
    slabs = VMEM((NODES, NODES, 8, LANES), jnp.float32)
    return pl.pallas_call(
        pressure_kernel,
        out_shape=jax.ShapeDtypeStruct((OWN // 2, NODES, NODES, 8, LANES), jnp.float32),
        in_specs=[pl.BlockSpec(memory_space=VMEM)] * 2,
        out_specs=pl.BlockSpec(memory_space=VMEM),
        scratch_shapes=[
            VMEM((4, NODES, NODES, 8, LANES), jnp.float32),
            VMEM((8, LANES), jnp.float32),
            field,
            field,
            field,
            field,
            slabs,
            slabs,
            VMEM((ITERS + 1, ELEMS, 2, 8, LANES), jnp.float32),
            VMEM((ITERS + 1, 2, 8, LANES), jnp.float32),
            DMA((ITERS + 1, ELEMS)),
            DMA((ITERS + 1, ELEMS)),
        ],
        compiler_params=pltpu.CompilerParams(collective_id=3, has_side_effects=True),
        name="pressure",
    )(predicted, metrics)


def on_device(velocity, radial_dx, radial_dy, around_dx, around_dy, jacobian):
    rows = velocity.transpose(0, 1, 3, 4, 2, 5).reshape(COMPONENTS * OWN * SQUARE * LAYERS, LANES)
    metrics = jnp.stack(
        [
            item.transpose(1, 2, 0, 3).reshape(SQUARE, LAYERS, LANES)
            for item in (radial_dx, radial_dy, around_dx, around_dy, jacobian)
        ]
    )
    metrics = jnp.concatenate([metrics, metrics], axis=2)
    packed = pack(rows).reshape(MODES, ROWS, LANES)
    received = exchange(packed, 1)
    answer = advect(received, metrics).reshape(MODES, ROWS, LANES)
    returned = exchange(answer, 2).reshape(MODES * ROWS, LANES)
    advection, predicted = unpack(returned, rows)
    pressure = pressure_of(predicted, metrics)
    advection = advection.reshape(COMPONENTS, OWN, NODES, NODES, LAYERS, LANES)
    advection = advection.transpose(0, 1, 4, 2, 3, 5)
    pressure = pressure.reshape(OWN // 2, NODES, NODES, 2, LAYERS, LANES)
    pressure = pressure.transpose(0, 3, 4, 1, 2, 5).reshape(OWN, LAYERS, NODES, NODES, LANES)
    return (advection, pressure)


def solution(mesh):
    metric = P(None, None, None, "elem")
    return jax.shard_map(
        on_device,
        mesh=mesh,
        in_specs=(P(None, "mode", None, None, None, "elem"),) + (metric,) * 5,
        out_specs=(P(None, "mode", None, None, None, "elem"), P("mode", None, None, None, "elem")),
        check_vma=False,
    )
```

```python
import functools
import itertools
import math

import jax
import jax.numpy as jnp
import numpy as np
from jax import lax
from jax.experimental import pallas as pl
from jax.experimental.pallas import tpu as pltpu
from jax.sharding import PartitionSpec as P

MESH = pl.DeviceIdType.MESH
NODES = 7
SQUARE = NODES * NODES
LAYERS = 4
ITERS = 3
COMPONENTS = 3
PLANES = 256
MODES = 64
OWN = PLANES // MODES
ELEMS = 4
LANES = 128
CELLS = COMPONENTS * SQUARE * LAYERS
CHUNKS = -(-CELLS // LANES)
PADDED = CHUNKS * LANES
HALF = MODES * CHUNKS * OWN
GROUPS = PADDED // 4

spanwise_wave = 2.0 * math.pi / 64.0
time_step = 0.1

VMEM = pltpu.VMEM
DMA = pltpu.SemaphoreType.DMA


def lobatto_rule(count):
    degree = count - 1
    points = np.cos(np.pi * np.arange(count) / degree)
    legendre = np.zeros((count, count))
    for sweep in range(60):
        legendre[:, 0] = 1.0
        legendre[:, 1] = points
        for order in range(2, count):
            legendre[:, order] = (
                (2 * order - 1) * points * legendre[:, order - 1]
                - (order - 1) * legendre[:, order - 2]
            ) / order
        points = points - (points * legendre[:, degree] - legendre[:, degree - 1]) / (
            count * legendre[:, degree]
        )
    legendre[:, 0] = 1.0
    legendre[:, 1] = points
    for order in range(2, count):
        legendre[:, order] = (
            (2 * order - 1) * points * legendre[:, order - 1] - (order - 1) * legendre[:, order - 2]
        ) / order
    weights = 2.0 / (degree * count * legendre[:, degree] ** 2)
    return (points[::-1].copy(), weights[::-1].copy())


def derivative_table():
    lobatto_nodes = lobatto_rule(NODES)[0]
    total = lobatto_nodes.shape[0]
    scales = np.ones(total)
    for column in range(total):
        for other in range(total):
            if other != column:
                scales[column] = scales[column] / (lobatto_nodes[column] - lobatto_nodes[other])
    table = np.zeros((total, total))
    for row in range(total):
        for column in range(total):
            if row != column:
                table[row, column] = (
                    scales[column] / scales[row] / (lobatto_nodes[row] - lobatto_nodes[column])
                )
        table[row, row] = -np.sum(table[row])
    return table


TABLE = derivative_table().astype(np.float32)
WEIGHTS = lobatto_rule(NODES)[1]


def split(value):
    high = value.astype(jnp.bfloat16)
    return (high, (value - high.astype(jnp.float32)).astype(jnp.bfloat16))


def constant_split(value):
    value = value.astype(np.float32)
    high = value.astype(jnp.bfloat16)
    return (high, (value - high.astype(np.float32)).astype(jnp.bfloat16))


def transform_tables():
    position = np.arange(PLANES)
    plane = np.arange(PLANES)
    order = plane // 2
    angle = 2.0 * np.pi / PLANES * ((position[:, None] * order[None, :]) % PLANES)
    is_sine = (plane % 2 == 1)[None, :]
    is_top = (plane == 1)[None, :]
    parity = np.cos(np.pi * (position % 2))[:, None]
    basis = np.where(is_top, parity, np.where(is_sine, np.sin(angle), np.cos(angle)))
    scaling = np.where(order == 0, 1.0, 2.0) / PLANES
    inverse = (basis * scaling[None, :]).T
    wave = (order * spanwise_wave)[None, :]
    slope = np.where(is_sine, wave * np.cos(angle), -wave * np.sin(angle))
    forward = np.concatenate([basis.T, slope.T], axis=1)
    turned = inverse.reshape(MODES, OWN, PLANES).transpose(1, 0, 2).reshape(PLANES, PLANES)
    return (*constant_split(forward), *constant_split(turned))


def swap_halves(value):
    return pltpu.roll(value, 4, value.ndim - 2)


def halves(first, second):
    lower = lax.broadcasted_iota(jnp.int32, first.shape, first.ndim - 2) < 4
    return (
        jnp.where(lower, first, swap_halves(second)),
        jnp.where(lower, swap_halves(first), second),
    )


def shifted(me, step):
    z, y, x = (me // 8, lax.rem(me // 2, 4), lax.rem(me, 2))
    dz, dy, dx = (step // 8, lax.rem(step // 2, 4), lax.rem(step, 2))
    return lax.rem(z + dz, 8) * 8 + lax.rem(y + dy, 4) * 2 + lax.rem(x + dx, 2)


def three_pass(first, second, dims):
    (a, b), (c, d) = (first, second)
    dot = functools.partial(
        lax.dot_general,
        dimension_numbers=(dims, ((), ())),
        preferred_element_type=jnp.float32,
    )
    return dot(a, c) + (dot(a, d) + dot(b, c))


def send_all(source, target, send_sem, receive_sem, me):
    def one(step, carry):
        other = shifted(me, step)
        pltpu.make_async_remote_copy(
            src_ref=source.at[other],
            dst_ref=target.at[me],
            send_sem=send_sem,
            recv_sem=receive_sem,
            device_id={"mode": other},
            device_id_type=MESH,
        ).start()
        return carry

    lax.fori_loop(1, MODES, one, 0)
    target[me] = source[me]


def wait_all(buffer, sem):
    others = buffer.at[pl.ds(0, MODES - 1)]
    pltpu.make_async_copy(others, others, sem).wait()


def step_kernel(velocity, radial_dx, radial_dy, around_dx, around_dy, jacobian,
                forward_high, forward_low, back_high, back_low, advection, out,
                rows, posted, got, answer, returned, local, values, result, predicted,
                fields, edges, geometry, tables, metrics, stiff, residual, direction, along,
                image_raw, radial_s, around_s, rims, posts,
                load_sem, store_sem, send_sem, receive_sem, rim_send_sem, rim_receive_sem):
    loads = [pltpu.make_async_copy(velocity, fields, load_sem.at[0])]
    for i, metric in enumerate((radial_dx, radial_dy, around_dx, around_dy, jacobian)):
        loads.append(pltpu.make_async_copy(metric, geometry.at[i], load_sem.at[1 + i]))
    for i, table in enumerate((forward_high, forward_low)):
        loads.append(pltpu.make_async_copy(table, tables.at[i], load_sem.at[6 + i]))
    for i, table in enumerate((back_high, back_low)):
        loads.append(pltpu.make_async_copy(table, edges.at[i], load_sem.at[8 + i]))
    for load in loads:
        load.start()
    me = lax.axis_index("mode")
    barrier = pltpu.get_barrier_semaphore()

    def greet(step, carry):
        pl.semaphore_signal(
            barrier, inc=1, device_id={"mode": shifted(me, step)}, device_id_type=MESH
        )
        return carry

    lax.fori_loop(1, MODES, greet, 0)
    here = lax.axis_index("elem")
    for step in range(1, ELEMS):
        pl.semaphore_signal(
            barrier, inc=1, device_id={"elem": lax.rem(here + step, ELEMS)}, device_id_type=MESH
        )
    loads[0].wait()

    outgoing = posted.reshape(2 * MODES * CHUNKS * OWN, LANES)
    for p in range(OWN):
        for c in range(COMPONENTS):
            start = (c * OWN + p) * SQUARE * LAYERS
            rows[p, pl.ds(c * SQUARE * LAYERS, SQUARE * LAYERS), :] = fields[
                pl.ds(start, SQUARE * LAYERS), :
            ]
        rows[p, pl.ds(CELLS, PADDED - CELLS), :] = jnp.zeros((PADDED - CELLS, LANES), jnp.float32)
        for k in range(CHUNKS):
            turned = rows[p, pl.ds(k * LANES, LANES), :].T
            for t in range(2):
                outgoing[pl.ds(t * HALF + k * OWN + p, MODES, stride=CHUNKS * OWN), :] = turned[
                    t * MODES : (t + 1) * MODES
                ]
    pl.semaphore_wait(barrier, MODES - 1 + ELEMS - 1)
    for t in range(2):
        send_all(posted.at[t], got.at[t], send_sem.at[0, t], receive_sem.at[0, t], me)

    for load in loads[1:]:
        load.wait()
    lane = lax.broadcasted_iota(jnp.int32, (SQUARE, LAYERS, LANES), 2)
    for t in range(2):
        for i in range(4):
            chosen = jnp.where(lane == me + t * MODES, geometry[i], 0.0)
            picked = jnp.sum(chosen, axis=2, keepdims=True)
            local[t, i] = jnp.broadcast_to(-picked, (SQUARE, LAYERS, LANES))

    sub = lax.broadcasted_iota(jnp.int32, (8, LANES), 0)
    lane = lax.broadcasted_iota(jnp.int32, (8, LANES), 1)
    layer = lax.rem(sub, 4)
    even = sub < 4
    inside = layer < LAYERS - 1
    above = layer > 0
    pairs = range(OWN // 2)
    nodes = range(NODES)

    for i in range(5):
        metrics[i] = jnp.concatenate([geometry[i]] * 2, axis=1)

    for a in nodes:
        for b in nodes:
            node = a * NODES + b
            rx, ry, ax, ay, jac = (metrics[i, node] for i in range(5))
            mass = float(np.float32(WEIGHTS[a] * WEIGHTS[b])) * jac
            stiff[0, a, b] = mass * (rx * rx + ry * ry)
            stiff[1, a, b] = mass * (rx * ax + ry * ay)
            stiff[2, a, b] = mass * (ax * ax + ay * ay)
            stiff[3, a, b] = mass

    zero = jnp.zeros((LAYERS, PLANES), jnp.float32)
    for g in range(COMPONENTS * SQUARE, GROUPS):
        result[g] = zero
    answers = answer.reshape(2 * MODES * CHUNKS * OWN, LANES)

    def advect(t, carry):
        wait_all(got.at[t], receive_sem.at[0, t])
        planes = jnp.concatenate(
            [got[t, :, k].reshape(PLANES, LANES) for k in range(CHUNKS)], axis=1
        )
        physical = three_pass(split(planes), (tables[0], tables[1]), ((0,), (0,)))
        values[...] = physical.reshape(GROUPS, LAYERS, 2 * PLANES)
        for a in range(NODES):
            for b in range(NODES):
                node = a * NODES + b
                mx, my, nx, ny = (
                    jnp.concatenate([local[t, i, node]] * 2, axis=1) for i in range(4)
                )
                u = values[node, :, :PLANES]
                v = values[SQUARE + node, :, :PLANES]
                w = values[2 * SQUARE + node, :, :PLANES]
                along = u * mx + v * my
                across = u * nx + v * ny
                for c in range(COMPONENTS):
                    radial, beside = (zero, zero)
                    for i in range(NODES):
                        radial += float(TABLE[a, i]) * values[c * SQUARE + i * NODES + b, :, :PLANES]
                        beside += float(TABLE[b, i]) * values[c * SQUARE + a * NODES + i, :, :PLANES]
                    slope = values[c * SQUARE + node, :, PLANES:]
                    result[c * SQUARE + node] = radial * along + beside * across - slope * w
        spectral = three_pass(
            (edges[0], edges[1]),
            split(result[...].reshape(PADDED, PLANES)),
            ((1,), (1,)),
        )
        for p in range(OWN):
            for k in range(CHUNKS):
                answers[pl.ds(t * HALF + k * OWN + p, MODES, stride=CHUNKS * OWN), :] = spectral[
                    p * MODES : (p + 1) * MODES, k * LANES : (k + 1) * LANES
                ]
        send_all(answer.at[t], returned.at[t], send_sem.at[1, t], receive_sem.at[1, t], me)
        return carry

    lax.fori_loop(0, 2, advect, 0)
    for t in range(2):
        wait_all(returned.at[t], receive_sem.at[1, t])

    incoming = returned.reshape(2 * MODES * CHUNKS * OWN, LANES)
    for p in range(OWN):
        for k in range(CHUNKS):
            block = jnp.concatenate(
                [
                    incoming[pl.ds(t * HALF + k * OWN + p, MODES, stride=CHUNKS * OWN), :]
                    for t in range(2)
                ],
                axis=0,
            )
            rows[p, pl.ds(k * LANES, LANES), :] = block.T
        for c in range(COMPONENTS):
            there = pl.ds((c * OWN + p) * SQUARE * LAYERS, SQUARE * LAYERS)
            own = pl.ds(c * SQUARE * LAYERS, SQUARE * LAYERS)
            term = rows[p, own, :]
            rows[p, own, :] = fields[there, :] + time_step * term
            fields[there, :] = term
    store = pltpu.make_async_copy(fields, advection, store_sem)
    store.start()
    for pair in range(OWN // 2):
        first, second = halves(
            rows[2 * pair].reshape(PADDED // 8, 8, LANES),
            rows[2 * pair + 1].reshape(PADDED // 8, 8, LANES),
        )
        for q in range(PADDED // 8):
            predicted[pair, 2 * q] = first[q]
            predicted[pair, 2 * q + 1] = second[q]

    orders = [(me * (OWN // 2) + pair).astype(jnp.float32) for pair in pairs]
    waves = [jnp.full((8, LANES), order) * spanwise_wave for order in orders]
    tops = [
        jnp.where((jnp.full((8, LANES), order) == 0.0) & (sub >= 4), float(PLANES // 2), order)
        * spanwise_wave
        for order in orders
    ]
    shifts = [top * top for top in tops]

    def radial_of(read, a):
        return functools.reduce(
            lambda x, y: x + y, [float(TABLE[a, i]) * read(i) for i in nodes]
        )

    def around_of(slab):
        return [
            functools.reduce(lambda x, y: x + y, [float(TABLE[b, i]) * slab[i] for i in nodes])
            for b in nodes
        ]

    for pair in pairs:
        wave = jnp.where(even, waves[pair], -waves[pair])
        for a in nodes:
            def component(c, i):
                return predicted[pair, pl.ds(c * SQUARE + i * NODES, NODES)]
            radial = [radial_of(functools.partial(component, c), a) for c in range(2)]
            beside = [around_of(component(c, a)) for c in range(2)]
            third = component(2, a)
            for b in nodes:
                node = a * NODES + b
                rx, ry, ax, ay = (metrics[i, node] for i in range(4))
                divergence = (
                    (rx * radial[0][b] + ax * beside[0][b])
                    + (ry * radial[1][b] + ay * beside[1][b])
                    + wave * swap_halves(third[b])
                )
                image_raw[pair, a, b] = -(stiff[3, a, b] * divergence) / time_step

    def across_layers():
        for pair in pairs:
            low, high = (image_raw[pair, 0], image_raw[pair, NODES - 1])
            other = [pltpu.roll(high[b], 1, 0) for b in nodes]
            this = [pltpu.roll(low[b], 7, 0) for b in nodes]
            for b in nodes:
                image_raw[pair, 0, b] = low[b] + jnp.where(above, other[b], 0.0)
                image_raw[pair, NODES - 1, b] = jnp.where(inside, high[b] + this[b], 0.0)

    def talk(phase, dots):
        first = jnp.zeros((8, LANES), jnp.float32)
        last = jnp.zeros((8, LANES), jnp.float32)
        if phase < ITERS:
            for pair in pairs:
                for a in nodes:
                    slot = pair * NODES + a
                    start = image_raw[pair, a, 0]
                    end = image_raw[pair, a, NODES - 1]
                    first = jnp.where(lane == slot, pltpu.roll(start, slot, 1) if slot else start, first)
                    last = jnp.where(lane == slot, pltpu.roll(end, slot + 1, 1), last)
        for index, dot in enumerate(dots):
            total = jnp.sum(dot, axis=1, keepdims=True)
            first = jnp.where(lane == 2 * 8 + index, total, first)
        posts[phase, 0] = first
        posts[phase, 1] = last
        rims[phase, here, 0] = first
        rims[phase, here, 1] = last
        copies = []
        for step in range(1, ELEMS):
            copy = pltpu.make_async_remote_copy(
                src_ref=posts.at[phase],
                dst_ref=rims.at[phase, here],
                send_sem=rim_send_sem.at[phase, step],
                recv_sem=rim_receive_sem.at[phase, step],
                device_id={"elem": lax.rem(here + step, ELEMS)},
                device_id_type=MESH,
            )
            copy.start()
            copies.append(copy)
        for copy in copies:
            copy.wait()
        total = (rims[phase, 0, 0] + rims[phase, 1, 0]) + (rims[phase, 2, 0] + rims[phase, 3, 0])
        sums = []
        for index in range(len(dots)):
            column = jnp.sum(jnp.where(lane == 2 * 8 + index, total, 0.0), axis=1, keepdims=True)
            column = jnp.broadcast_to(column, (8, LANES))
            lower = jnp.sum(jnp.where(even, column, 0.0), axis=0, keepdims=True)
            upper = jnp.sum(jnp.where(even, 0.0, column), axis=0, keepdims=True)
            sums.append(jnp.where(even, lower, upper))
        right = rims[phase, lax.rem(here + 1, ELEMS), 0]
        left = rims[phase, lax.rem(here + ELEMS - 1, ELEMS), 1]
        return (sums, left, right)

    def across_columns(pair, a, left, right):
        slot = pair * NODES + a
        start = image_raw[pair, a, 0]
        end = image_raw[pair, a, NODES - 1]
        after = jnp.where(
            lane == LANES - 1, pltpu.roll(right, LANES - 1 - slot, 1), pltpu.roll(start, LANES - 1, 1)
        )
        before = jnp.where(
            lane == 0, pltpu.roll(left, (LANES - slot) % LANES, 1) if slot else left, pltpu.roll(end, 1, 1)
        )
        return (start + before, end + after)

    across_layers()
    _, left, right = talk(0, [])
    for pair in pairs:
        for a in nodes:
            start, end = across_columns(pair, a, left, right)
            for b in nodes:
                value = start if b == 0 else end if b == NODES - 1 else image_raw[pair, a, b]
                residual[pair, a, b] = value

    weight_a = [
        jnp.where(above, 0.5, 1.0) if a == 0 else jnp.where(inside, 0.5, 0.0) if a == NODES - 1 else None
        for a in nodes
    ]

    gamma_old = [None, None]
    inner_old = [None, None]
    for turn in range(ITERS):
        dots = []
        for pair in pairs:
            norm = jnp.zeros((8, LANES), jnp.float32)
            for a in nodes:
                slab = residual[pair, a]
                radial = radial_of(lambda i: residual[pair, i], a)
                beside = around_of(slab)
                row = jnp.zeros((8, LANES), jnp.float32)
                for b in nodes:
                    g11, g12, g22 = (stiff[i, a, b] for i in range(3))
                    radial_s[a, b] = g11 * radial[b] + g12 * beside[b]
                    around_s[a, b] = g12 * radial[b] + g22 * beside[b]
                    square = slab[b] * slab[b]
                    row = row + (0.5 * square if b in (0, NODES - 1) else square)
                norm = norm + (row if weight_a[a] is None else row * weight_a[a])
            product = jnp.zeros((8, LANES), jnp.float32)
            for a in nodes:
                spread = functools.reduce(
                    lambda x, y: x + y, [float(TABLE[i, a]) * radial_s[i] for i in nodes]
                )
                slab = around_s[a]
                for b in nodes:
                    beside = functools.reduce(
                        lambda x, y: x + y, [float(TABLE[j, b]) * slab[j] for j in nodes]
                    )
                    here_now = residual[pair, a, b]
                    value = spread[b] + beside + shifts[pair] * stiff[3, a, b] * here_now
                    image_raw[pair, a, b] = value
                    product = product + here_now * value
            dots += [norm, product]
        if turn < ITERS - 1:
            across_layers()
        sums, left, right = talk(turn + 1, dots)
        for pair in pairs:
            gamma, delta = (sums[2 * pair], sums[2 * pair + 1])
            if turn == 0:
                beta, inner = (None, delta)
            else:
                beta = gamma / gamma_old[pair]
                inner = delta - beta * beta * inner_old[pair]
            alpha = gamma / inner
            gamma_old[pair], inner_old[pair] = (gamma, inner)
            for a in nodes:
                if turn < ITERS - 1:
                    start, end = across_columns(pair, a, left, right)
                for b in nodes:
                    now = residual[pair, a, b]
                    if turn:
                        now = now + beta * direction[pair, a, b]
                    step = alpha * now
                    total = step if turn == 0 else predicted[pair, a * NODES + b] + step
                    if turn == ITERS - 1:
                        for h in range(2):
                            out[2 * pair + h, a * NODES + b] = total[h * LAYERS : (h + 1) * LAYERS]
                    else:
                        predicted[pair, a * NODES + b] = total
                    if turn < ITERS - 1:
                        direction[pair, a, b] = now
                        image = start if b == 0 else end if b == NODES - 1 else image_raw[pair, a, b]
                        if turn:
                            image = image + beta * along[pair, a, b]
                        along[pair, a, b] = image
                        residual[pair, a, b] = residual[pair, a, b] - alpha * image

    store.wait()
    for t in range(2):
        wait_all(posted.at[t], send_sem.at[0, t])
        wait_all(answer.at[t], send_sem.at[1, t])


def step_of(velocity, *metrics):
    tables = transform_tables()
    blocks = VMEM((2, MODES, CHUNKS, OWN, LANES), jnp.float32)
    field = VMEM((OWN // 2, NODES, NODES, 8, LANES), jnp.float32)
    slabs = VMEM((NODES, NODES, 8, LANES), jnp.float32)
    return pl.pallas_call(
        step_kernel,
        out_shape=(
            jax.ShapeDtypeStruct(velocity.shape, jnp.float32),
            jax.ShapeDtypeStruct((OWN, SQUARE, LAYERS, LANES), jnp.float32),
        ),
        in_specs=[pl.BlockSpec(memory_space=pltpu.HBM)] * 10,
        out_specs=(pl.BlockSpec(memory_space=pltpu.HBM), pl.BlockSpec(memory_space=VMEM)),
        scratch_shapes=[
            VMEM((OWN, PADDED, LANES), jnp.float32),
            blocks,
            blocks,
            blocks,
            blocks,
            VMEM((2, 4, SQUARE, LAYERS, LANES), jnp.float32),
            VMEM((GROUPS, LAYERS, 2 * PLANES), jnp.float32),
            VMEM((GROUPS, LAYERS, PLANES), jnp.float32),
            VMEM((OWN // 2, GROUPS, 8, LANES), jnp.float32),
            VMEM(velocity.shape, jnp.float32),
            VMEM((2, PLANES, PLANES), jnp.bfloat16),
            VMEM((5, SQUARE, LAYERS, LANES), jnp.float32),
            VMEM((2, PLANES, 2 * PLANES), jnp.bfloat16),
            VMEM((5, SQUARE, 8, LANES), jnp.float32),
            VMEM((4, NODES, NODES, 8, LANES), jnp.float32),
            field,
            field,
            field,
            field,
            slabs,
            slabs,
            VMEM((ITERS + 1, ELEMS, 2, 8, LANES), jnp.float32),
            VMEM((ITERS + 1, 2, 8, LANES), jnp.float32),
            DMA((10,)),
            DMA,
            DMA((2, 2)),
            DMA((2, 2)),
            DMA((ITERS + 1, ELEMS)),
            DMA((ITERS + 1, ELEMS)),
        ],
        compiler_params=pltpu.CompilerParams(
            collective_id=1, has_side_effects=True, vmem_limit_bytes=60 << 20
        ),
        name="step",
    )(velocity, *metrics, *(jnp.asarray(t) for t in tables))


def on_device(velocity, radial_dx, radial_dy, around_dx, around_dy, jacobian):
    rows = velocity.transpose(0, 1, 3, 4, 2, 5).reshape(COMPONENTS * OWN * SQUARE * LAYERS, LANES)
    metrics = [
        item.transpose(1, 2, 0, 3).reshape(SQUARE, LAYERS, LANES)
        for item in (radial_dx, radial_dy, around_dx, around_dy, jacobian)
    ]
    advection, pressure = step_of(rows, *metrics)
    advection = advection.reshape(COMPONENTS, OWN, NODES, NODES, LAYERS, LANES)
    pressure = pressure.reshape(OWN, NODES, NODES, LAYERS, LANES)
    return (advection.transpose(0, 1, 4, 2, 3, 5), pressure.transpose(0, 3, 1, 2, 4))


def solution(mesh):
    metric = P(None, None, None, "elem")
    return jax.shard_map(
        on_device,
        mesh=mesh,
        in_specs=(P(None, "mode", None, None, None, "elem"),) + (metric,) * 5,
        out_specs=(P(None, "mode", None, None, None, "elem"), P("mode", None, None, None, "elem")),
        check_vma=False,
    )
```

```python
import functools
import itertools
import math

import jax
import jax.numpy as jnp
import numpy as np
from jax import lax
from jax.experimental import pallas as pl
from jax.experimental.pallas import tpu as pltpu
from jax.sharding import PartitionSpec as P

MESH = pl.DeviceIdType.MESH
NODES = 7
SQUARE = NODES * NODES
LAYERS = 4
ITERS = 3
COMPONENTS = 3
PLANES = 256
MODES = 64
OWN = PLANES // MODES
ELEMS = 4
LANES = 128
CELLS = COMPONENTS * SQUARE * LAYERS
CHUNKS = -(-CELLS // LANES)
PADDED = CHUNKS * LANES
FULL = CELLS // LANES
REST = CELLS - FULL * LANES
SPARE = LANES - REST
TAIL = REST - SPARE
LARGE = FULL * OWN + 3
SMALL = FULL * OWN + 2
GROUPS = PADDED // 4

spanwise_wave = 2.0 * math.pi / 64.0
time_step = 0.1

VMEM = pltpu.VMEM
DMA = pltpu.SemaphoreType.DMA


def lobatto_rule(count):
    degree = count - 1
    points = np.cos(np.pi * np.arange(count) / degree)
    legendre = np.zeros((count, count))
    for sweep in range(60):
        legendre[:, 0] = 1.0
        legendre[:, 1] = points
        for order in range(2, count):
            legendre[:, order] = (
                (2 * order - 1) * points * legendre[:, order - 1]
                - (order - 1) * legendre[:, order - 2]
            ) / order
        points = points - (points * legendre[:, degree] - legendre[:, degree - 1]) / (
            count * legendre[:, degree]
        )
    legendre[:, 0] = 1.0
    legendre[:, 1] = points
    for order in range(2, count):
        legendre[:, order] = (
            (2 * order - 1) * points * legendre[:, order - 1] - (order - 1) * legendre[:, order - 2]
        ) / order
    weights = 2.0 / (degree * count * legendre[:, degree] ** 2)
    return (points[::-1].copy(), weights[::-1].copy())


def derivative_table():
    lobatto_nodes = lobatto_rule(NODES)[0]
    total = lobatto_nodes.shape[0]
    scales = np.ones(total)
    for column in range(total):
        for other in range(total):
            if other != column:
                scales[column] = scales[column] / (lobatto_nodes[column] - lobatto_nodes[other])
    table = np.zeros((total, total))
    for row in range(total):
        for column in range(total):
            if row != column:
                table[row, column] = (
                    scales[column] / scales[row] / (lobatto_nodes[row] - lobatto_nodes[column])
                )
        table[row, row] = -np.sum(table[row])
    return table


TABLE = derivative_table().astype(np.float32)
WEIGHTS = lobatto_rule(NODES)[1]


def split(value):
    high = value.astype(jnp.bfloat16)
    return (high, (value - high.astype(jnp.float32)).astype(jnp.bfloat16))


def constant_split(value):
    value = value.astype(np.float32)
    high = value.astype(jnp.bfloat16)
    return (high, (value - high.astype(np.float32)).astype(jnp.bfloat16))


def transform_tables():
    position = np.arange(PLANES)
    plane = np.arange(PLANES)
    order = plane // 2
    angle = 2.0 * np.pi / PLANES * ((position[:, None] * order[None, :]) % PLANES)
    is_sine = (plane % 2 == 1)[None, :]
    is_top = (plane == 1)[None, :]
    parity = np.cos(np.pi * (position % 2))[:, None]
    basis = np.where(is_top, parity, np.where(is_sine, np.sin(angle), np.cos(angle)))
    scaling = np.where(order == 0, 1.0, 2.0) / PLANES
    inverse = (basis * scaling[None, :]).T
    wave = (order * spanwise_wave)[None, :]
    slope = np.where(is_sine, wave * np.cos(angle), -wave * np.sin(angle))
    forward = np.concatenate([basis.T, slope.T], axis=1)
    forward = forward.reshape(MODES, OWN, 2 * PLANES).transpose(1, 0, 2).reshape(PLANES, 2 * PLANES)
    turned = inverse.reshape(MODES, OWN, PLANES).transpose(1, 0, 2).reshape(PLANES, PLANES)
    return (*constant_split(forward), *constant_split(turned))


def contract(matrix, field):
    last, half = (NODES - 1, NODES // 2)
    even = [field[j] + field[last - j] for j in range(half)]
    odd = [field[j] - field[last - j] for j in range(half)]

    def total(terms):
        return functools.reduce(lambda x, y: x + y, terms)

    out = [None] * NODES
    for i in range(half):
        minus = [0.5 * (float(matrix[i, j]) - float(matrix[i, last - j])) for j in range(half)]
        plus = [0.5 * (float(matrix[i, j]) + float(matrix[i, last - j])) for j in range(half)]
        p = total([minus[j] * odd[j] for j in range(half)])
        q = total([plus[j] * even[j] for j in range(half)] + [float(matrix[i, half]) * field[half]])
        out[i], out[last - i] = (p + q, p - q)
    out[half] = total([float(matrix[half, j]) * odd[j] for j in range(half)])
    return out


def swap_halves(value):
    return pltpu.roll(value, 4, value.ndim - 2)


def halves(first, second):
    lower = lax.broadcasted_iota(jnp.int32, first.shape, first.ndim - 2) < 4
    return (
        jnp.where(lower, first, swap_halves(second)),
        jnp.where(lower, swap_halves(first), second),
    )


def partner(me, step):
    z, y, x = (me // 8, lax.rem(me // 2, 4), lax.rem(me, 2))
    turn_z, rest = (step // 8, 7 - lax.rem(step, 8))
    dz = 4 + turn_z // 2 - lax.rem(turn_z, 2) * (turn_z // 2 + (turn_z + 1) // 2)
    dy, dx = (rest // 2, lax.rem(rest, 2))
    return lax.rem(z + dz, 8) * 8 + lax.rem(y + dy, 4) * 2 + lax.rem(x + dx, 2)


def three_pass(first, second, dims):
    (a, b), (c, d) = (first, second)
    dot = functools.partial(
        lax.dot_general,
        dimension_numbers=(dims, ((), ())),
        preferred_element_type=jnp.float32,
    )
    return dot(a, c) + (dot(a, d) + dot(b, c))


def rows_of(ref):
    return ref.reshape(MODES * ref.shape[1], LANES)


def put(ref, row, value):
    rows_of(ref)[pl.ds(row, MODES, stride=ref.shape[1]), :] = value


def take(ref, row):
    return rows_of(ref)[pl.ds(row, MODES, stride=ref.shape[1]), :]


def before(bound, first, second):
    lane = lax.broadcasted_iota(jnp.int32, first.shape, 1)
    return jnp.where(lane < bound, first, second)


def turn(value, amount):
    return pltpu.roll(value, amount % LANES, 1)


def put_large(ref, x, small_rest):
    put(ref, FULL * OWN, before(REST, x[0], turn(x[3], REST)))
    put(ref, FULL * OWN + 1, before(REST, x[1], turn(x[3], TAIL)))
    rest = before(REST + TAIL, turn(small_rest[0], TAIL), turn(small_rest[1], 2 * TAIL))
    put(ref, FULL * OWN + 2, before(REST, x[2], rest))


def put_small(ref, y):
    put(ref, FULL * OWN, before(REST, y[0], turn(y[3], REST)))
    put(ref, FULL * OWN + 1, before(REST, y[1], turn(y[2], REST)))


def take_large(ref):
    x = [take(ref, FULL * OWN + i) for i in range(3)]
    return x + [before(SPARE, turn(x[0], -REST), turn(x[1], -TAIL))]


def take_small(ref, large):
    y = [take(ref, FULL * OWN + i) for i in range(2)]
    rest = take(large, FULL * OWN + 2)
    return y + [
        before(SPARE, turn(y[1], -REST), turn(rest, -TAIL)),
        before(SPARE, turn(y[0], -REST), turn(rest, -2 * TAIL)),
    ]


def send_all(source, target, send_sem, receive_sem, me):
    def one(step, carry):
        other = partner(me, step)
        pltpu.make_async_remote_copy(
            src_ref=source.at[other],
            dst_ref=target.at[me],
            send_sem=send_sem,
            recv_sem=receive_sem,
            device_id={"mode": other},
            device_id_type=MESH,
        ).start()
        return carry

    lax.fori_loop(0, MODES - 1, one, 0)
    target[me] = source[me]


def wait_all(buffer, sem):
    others = buffer.at[pl.ds(0, MODES - 1)]
    pltpu.make_async_copy(others, others, sem).wait()


def step_kernel(velocity, radial_dx, radial_dy, around_dx, around_dy, jacobian,
                forward_high, forward_low, back_high, back_low, advection, out,
                rows, posted_0, posted_1, got_0, got_1, answer_0, answer_1, returned_0, returned_1, local, values, result, predicted,
                fields, edges, geometry, tables, metrics, stiff, residual, direction, carried,
                image_raw, radial_s, around_s, rims, posts,
                load_sem, send_sem, receive_sem, rim_send_sem, rim_receive_sem):
    loads = [pltpu.make_async_copy(velocity, fields, load_sem.at[0])]
    for i, metric in enumerate((radial_dx, radial_dy, around_dx, around_dy, jacobian)):
        loads.append(pltpu.make_async_copy(metric, geometry.at[i], load_sem.at[1 + i]))
    for i, table in enumerate((forward_high, forward_low)):
        loads.append(pltpu.make_async_copy(table, tables.at[i], load_sem.at[6 + i]))
    for i, table in enumerate((back_high, back_low)):
        loads.append(pltpu.make_async_copy(table, edges.at[i], load_sem.at[8 + i]))
    loads[0].start()
    me = lax.axis_index("mode")
    barrier = pltpu.get_barrier_semaphore()

    def greet(step, carry):
        pl.semaphore_signal(
            barrier, inc=1, device_id={"mode": partner(me, step)}, device_id_type=MESH
        )
        return carry

    lax.fori_loop(0, MODES - 1, greet, 0)
    here = lax.axis_index("elem")
    for step in range(1, ELEMS):
        pl.semaphore_signal(
            barrier, inc=1, device_id={"elem": lax.rem(here + step, ELEMS)}, device_id_type=MESH
        )
    loads[0].wait()
    for load in loads[1:]:
        load.start()

    posted, got = ((posted_0, posted_1), (got_0, got_1))
    answer, returned = ((answer_0, answer_1), (returned_0, returned_1))
    last = ([], [])
    for p in range(OWN):
        for c in range(COMPONENTS):
            start = (c * OWN + p) * SQUARE * LAYERS
            rows[p, pl.ds(c * SQUARE * LAYERS, SQUARE * LAYERS), :] = fields[
                pl.ds(start, SQUARE * LAYERS), :
            ]
        rows[p, pl.ds(CELLS, PADDED - CELLS), :] = jnp.zeros((PADDED - CELLS, LANES), jnp.float32)
        for k in range(CHUNKS):
            turned = rows[p, pl.ds(k * LANES, LANES), :].T
            for t in range(2):
                part = turned[t * MODES : (t + 1) * MODES]
                if k < FULL:
                    put(posted[t], k * OWN + p, part)
                else:
                    last[t].append(part)
    put_large(posted_0, last[0], last[1][2:])
    put_small(posted_1, last[1])
    pl.semaphore_wait(barrier, MODES - 1 + ELEMS - 1)
    for t in range(2):
        send_all(posted[t], got[t], send_sem.at[0, t], receive_sem.at[0, t], me)

    for load in loads[1:]:
        load.wait()
    lane = lax.broadcasted_iota(jnp.int32, (SQUARE, LAYERS, LANES), 2)
    for t in range(2):
        for i in range(4):
            chosen = jnp.where(lane == me + t * MODES, geometry[i], 0.0)
            picked = jnp.sum(chosen, axis=2, keepdims=True)
            local[t, i] = jnp.broadcast_to(-picked, (SQUARE, LAYERS, LANES))

    sub = lax.broadcasted_iota(jnp.int32, (8, LANES), 0)
    lane = lax.broadcasted_iota(jnp.int32, (8, LANES), 1)
    layer = lax.rem(sub, 4)
    even = sub < 4
    inside = layer < LAYERS - 1
    above = layer > 0
    pairs = range(OWN // 2)
    nodes = range(NODES)

    for i in range(5):
        metrics[i] = jnp.concatenate([geometry[i]] * 2, axis=1)

    for a in nodes:
        for b in nodes:
            node = a * NODES + b
            rx, ry, ax, ay, jac = (metrics[i, node] for i in range(5))
            mass = float(np.float32(WEIGHTS[a] * WEIGHTS[b])) * jac
            stiff[0, a, b] = mass * (rx * rx + ry * ry)
            stiff[1, a, b] = mass * (rx * ax + ry * ay)
            stiff[2, a, b] = mass * (ax * ax + ay * ay)
            stiff[3, a, b] = mass

    zero = jnp.zeros((LAYERS, PLANES), jnp.float32)
    for g in range(COMPONENTS * SQUARE, GROUPS):
        result[g] = zero
    small_rest = []
    for t in range(2):
        wait_all(got[t], receive_sem.at[0, t])
        rest = take_small(got_1, got_0) if t else take_large(got_0)
        planes = jnp.concatenate(
            [
                jnp.concatenate([take(got[t], k * OWN + p) for p in range(OWN)], axis=0)
                for k in range(FULL)
            ]
            + [jnp.concatenate(rest, axis=0)],
            axis=1,
        )
        physical = three_pass(split(planes), (tables[0], tables[1]), ((0,), (0,)))
        values[...] = physical.reshape(GROUPS, LAYERS, 2 * PLANES)
        for a in range(NODES):
            for b in range(NODES):
                node = a * NODES + b
                mx, my, nx, ny = (
                    jnp.concatenate([local[t, i, node]] * 2, axis=1) for i in range(4)
                )
                u = values[node, :, :PLANES]
                v = values[SQUARE + node, :, :PLANES]
                w = values[2 * SQUARE + node, :, :PLANES]
                along = u * mx + v * my
                across = u * nx + v * ny
                for c in range(COMPONENTS):
                    radial, beside = (zero, zero)
                    for i in range(NODES):
                        radial += float(TABLE[a, i]) * values[c * SQUARE + i * NODES + b, :, :PLANES]
                        beside += float(TABLE[b, i]) * values[c * SQUARE + a * NODES + i, :, :PLANES]
                    slope = values[c * SQUARE + node, :, PLANES:]
                    result[c * SQUARE + node] = radial * along + beside * across - slope * w
        spectral = three_pass(
            (edges[0], edges[1]),
            split(result[...].reshape(PADDED, PLANES)),
            ((1,), (1,)),
        )
        last = []
        for p in range(OWN):
            part = spectral[p * MODES : (p + 1) * MODES]
            for k in range(FULL):
                put(answer[t], k * OWN + p, part[:, k * LANES : (k + 1) * LANES])
            last.append(part[:, FULL * LANES :])
        if t:
            put_large(answer_1, last, small_rest)
        else:
            put_small(answer_0, last)
            small_rest = last[2:]
        send_all(answer[t], returned[t], send_sem.at[1, t], receive_sem.at[1, t], me)
    for t in range(2):
        wait_all(returned[t], receive_sem.at[1, t])

    rest = (take_small(returned_0, returned_1), take_large(returned_1))
    for p in range(OWN):
        for k in range(CHUNKS):
            block = jnp.concatenate(
                [
                    take(returned[t], k * OWN + p) if k < FULL else rest[t][p]
                    for t in range(2)
                ],
                axis=0,
            )
            rows[p, pl.ds(k * LANES, LANES), :] = block.T
        for c in range(COMPONENTS):
            there = pl.ds((c * OWN + p) * SQUARE * LAYERS, SQUARE * LAYERS)
            own = pl.ds(c * SQUARE * LAYERS, SQUARE * LAYERS)
            term = rows[p, own, :]
            rows[p, own, :] = fields[there, :] + time_step * term
            advection[there, :] = term
    for pair in range(OWN // 2):
        first, second = halves(
            rows[2 * pair].reshape(PADDED // 8, 8, LANES),
            rows[2 * pair + 1].reshape(PADDED // 8, 8, LANES),
        )
        for q in range(PADDED // 8):
            predicted[pair, 2 * q] = first[q]
            predicted[pair, 2 * q + 1] = second[q]

    orders = [(me * (OWN // 2) + pair).astype(jnp.float32) for pair in pairs]
    waves = [jnp.full((8, LANES), order) * spanwise_wave for order in orders]
    tops = [
        jnp.where((jnp.full((8, LANES), order) == 0.0) & (sub >= 4), float(PLANES // 2), order)
        * spanwise_wave
        for order in orders
    ]
    shifts = [top * top for top in tops]

    for pair in pairs:
        wave = jnp.where(even, waves[pair], -waves[pair])
        for b in nodes:
            for c, kept in enumerate((radial_s, around_s)):
                radial = contract(
                    TABLE, [predicted[pair, c * SQUARE + a * NODES + b] for a in nodes]
                )
                for a in nodes:
                    kept[a, b] = radial[a]
        for a in nodes:
            beside = [
                contract(TABLE, [predicted[pair, c * SQUARE + a * NODES + b] for b in nodes])
                for c in range(2)
            ]
            for b in nodes:
                node = a * NODES + b
                rx, ry, ax, ay = (metrics[i, node] for i in range(4))
                divergence = (
                    (rx * radial_s[a, b] + ax * beside[0][b])
                    + (ry * around_s[a, b] + ay * beside[1][b])
                    + wave * swap_halves(predicted[pair, 2 * SQUARE + node])
                )
                image_raw[pair, a, b] = (stiff[3, a, b] * divergence) * (-1.0 / time_step)

    def across_layers():
        for pair in pairs:
            low, high = (image_raw[pair, 0], image_raw[pair, NODES - 1])
            other = [pltpu.roll(high[b], 1, 0) for b in nodes]
            this = [pltpu.roll(low[b], 7, 0) for b in nodes]
            for b in nodes:
                image_raw[pair, 0, b] = low[b] + jnp.where(above, other[b], 0.0)
                image_raw[pair, NODES - 1, b] = jnp.where(inside, high[b] + this[b], 0.0)

    def talk(phase, dots):
        first = jnp.zeros((8, LANES), jnp.float32)
        last = jnp.zeros((8, LANES), jnp.float32)
        if phase < ITERS:
            for pair in pairs:
                for a in nodes:
                    slot = pair * NODES + a
                    start = image_raw[pair, a, 0]
                    end = image_raw[pair, a, NODES - 1]
                    first = jnp.where(lane == slot, pltpu.roll(start, slot, 1) if slot else start, first)
                    last = jnp.where(lane == slot, pltpu.roll(end, slot + 1, 1), last)
        for index, dot in enumerate(dots):
            total = jnp.sum(dot, axis=1, keepdims=True)
            first = jnp.where(lane == 2 * 8 + index, total, first)
        posts[phase, 0] = first
        posts[phase, 1] = last
        rims[phase, here, 0] = first
        rims[phase, here, 1] = last
        copies = []
        for step in range(1, ELEMS):
            copy = pltpu.make_async_remote_copy(
                src_ref=posts.at[phase],
                dst_ref=rims.at[phase, here],
                send_sem=rim_send_sem.at[phase, step],
                recv_sem=rim_receive_sem.at[phase, step],
                device_id={"elem": lax.rem(here + step, ELEMS)},
                device_id_type=MESH,
            )
            copy.start()
            copies.append(copy)
        for copy in copies:
            copy.wait()
        total = (rims[phase, 0, 0] + rims[phase, 1, 0]) + (rims[phase, 2, 0] + rims[phase, 3, 0])
        sums = []
        for index in range(len(dots)):
            column = jnp.sum(jnp.where(lane == 2 * 8 + index, total, 0.0), axis=1, keepdims=True)
            column = jnp.broadcast_to(column, (8, LANES))
            lower = jnp.sum(jnp.where(even, column, 0.0), axis=0, keepdims=True)
            upper = jnp.sum(jnp.where(even, 0.0, column), axis=0, keepdims=True)
            sums.append(jnp.where(even, lower, upper))
        right = rims[phase, lax.rem(here + 1, ELEMS), 0]
        left = rims[phase, lax.rem(here + ELEMS - 1, ELEMS), 1]
        return (sums, left, right)

    def across_columns(pair, a, left, right):
        slot = pair * NODES + a
        start = image_raw[pair, a, 0]
        end = image_raw[pair, a, NODES - 1]
        after = jnp.where(
            lane == LANES - 1, pltpu.roll(right, LANES - 1 - slot, 1), pltpu.roll(start, LANES - 1, 1)
        )
        before = jnp.where(
            lane == 0, pltpu.roll(left, (LANES - slot) % LANES, 1) if slot else left, pltpu.roll(end, 1, 1)
        )
        return (start + before, end + after)

    across_layers()
    _, left, right = talk(0, [])
    for pair in pairs:
        for a in nodes:
            start, end = across_columns(pair, a, left, right)
            for b in nodes:
                value = start if b == 0 else end if b == NODES - 1 else image_raw[pair, a, b]
                residual[pair, a, b] = value

    weight_a = [
        jnp.where(above, 0.5, 1.0) if a == 0 else jnp.where(inside, 0.5, 0.0) if a == NODES - 1 else None
        for a in nodes
    ]

    gamma_old = [None, None]
    inner_old = [None, None]
    for turn in range(ITERS):
        dots = []
        for pair in pairs:
            for b in nodes:
                radial = contract(TABLE, [residual[pair, a, b] for a in nodes])
                for a in nodes:
                    radial_s[a, b] = radial[a]
            norm = jnp.zeros((8, LANES), jnp.float32)
            for a in nodes:
                slab = [residual[pair, a, b] for b in nodes]
                beside = contract(TABLE, slab)
                spread = []
                for b in nodes:
                    g11, g12, g22 = (stiff[i, a, b] for i in range(3))
                    radial = radial_s[a, b]
                    radial_s[a, b] = g11 * radial + g12 * beside[b]
                    spread.append(g12 * radial + g22 * beside[b])
                spread = contract(TABLE.T, spread)
                squares = [item * item for item in slab]
                row = 0.5 * (squares[0] + squares[NODES - 1])
                for b in nodes:
                    image_raw[pair, a, b] = spread[b] + shifts[pair] * stiff[3, a, b] * slab[b]
                    if 0 < b < NODES - 1:
                        row = row + squares[b]
                norm = norm + (row if weight_a[a] is None else row * weight_a[a])
            product = jnp.zeros((8, LANES), jnp.float32)
            for b in nodes:
                radial = contract(TABLE.T, [radial_s[a, b] for a in nodes])
                for a in nodes:
                    value = image_raw[pair, a, b] + radial[a]
                    image_raw[pair, a, b] = value
                    product = product + residual[pair, a, b] * value
            dots += [norm, product]
        if turn < ITERS - 1:
            across_layers()
        sums, left, right = talk(turn + 1, dots)
        for pair in pairs:
            gamma, delta = (sums[2 * pair], sums[2 * pair + 1])
            if turn == 0:
                beta, inner = (None, delta)
            else:
                beta = gamma / gamma_old[pair]
                inner = delta - beta * beta * inner_old[pair]
            alpha = gamma / inner
            gamma_old[pair], inner_old[pair] = (gamma, inner)
            for a in nodes:
                if turn < ITERS - 1:
                    start, end = across_columns(pair, a, left, right)
                for b in nodes:
                    now = residual[pair, a, b]
                    if turn:
                        now = now + beta * direction[pair, a, b]
                    step = alpha * now
                    total = step if turn == 0 else predicted[pair, a * NODES + b] + step
                    if turn == ITERS - 1:
                        for h in range(2):
                            out[2 * pair + h, a * NODES + b] = total[h * LAYERS : (h + 1) * LAYERS]
                    else:
                        predicted[pair, a * NODES + b] = total
                    if turn < ITERS - 1:
                        direction[pair, a, b] = now
                        image = start if b == 0 else end if b == NODES - 1 else image_raw[pair, a, b]
                        if turn:
                            image = image + beta * carried[pair, a, b]
                        carried[pair, a, b] = image
                        residual[pair, a, b] = residual[pair, a, b] - alpha * image

    for t in range(2):
        wait_all(posted[t], send_sem.at[0, t])
        wait_all(answer[t], send_sem.at[1, t])


def step_of(velocity, *metrics):
    tables = transform_tables()
    large, small = (VMEM((MODES, rows, 1, LANES), jnp.float32) for rows in (LARGE, SMALL))
    field = VMEM((OWN // 2, NODES, NODES, 8, LANES), jnp.float32)
    slabs = VMEM((NODES, NODES, 8, LANES), jnp.float32)
    return pl.pallas_call(
        step_kernel,
        out_shape=(
            jax.ShapeDtypeStruct(velocity.shape, jnp.float32),
            jax.ShapeDtypeStruct((OWN, SQUARE, LAYERS, LANES), jnp.float32),
        ),
        in_specs=[pl.BlockSpec(memory_space=pltpu.HBM)] * 10,
        out_specs=(pl.BlockSpec(memory_space=VMEM),) * 2,
        scratch_shapes=[
            VMEM((OWN, PADDED, LANES), jnp.float32),
            large,
            small,
            large,
            small,
            small,
            large,
            small,
            large,
            VMEM((2, 4, SQUARE, LAYERS, LANES), jnp.float32),
            VMEM((GROUPS, LAYERS, 2 * PLANES), jnp.float32),
            VMEM((GROUPS, LAYERS, PLANES), jnp.float32),
            VMEM((OWN // 2, GROUPS, 8, LANES), jnp.float32),
            VMEM(velocity.shape, jnp.float32),
            VMEM((2, PLANES, PLANES), jnp.bfloat16),
            VMEM((5, SQUARE, LAYERS, LANES), jnp.float32),
            VMEM((2, PLANES, 2 * PLANES), jnp.bfloat16),
            VMEM((5, SQUARE, 8, LANES), jnp.float32),
            VMEM((4, NODES, NODES, 8, LANES), jnp.float32),
            field,
            field,
            field,
            field,
            slabs,
            slabs,
            VMEM((ITERS + 1, ELEMS, 2, 8, LANES), jnp.float32),
            VMEM((ITERS + 1, 2, 8, LANES), jnp.float32),
            DMA((10,)),
            DMA((2, 2)),
            DMA((2, 2)),
            DMA((ITERS + 1, ELEMS)),
            DMA((ITERS + 1, ELEMS)),
        ],
        compiler_params=pltpu.CompilerParams(
            collective_id=1, has_side_effects=True, vmem_limit_bytes=40 << 20
        ),
        name="step",
    )(
        *(
            pltpu.with_memory_space_constraint(item, pltpu.HBM)
            for item in (velocity, *metrics, *(jnp.asarray(t) for t in tables))
        )
    )


def on_device(velocity, radial_dx, radial_dy, around_dx, around_dy, jacobian):
    rows = velocity.transpose(0, 1, 3, 4, 2, 5).reshape(COMPONENTS * OWN * SQUARE * LAYERS, LANES)
    metrics = [
        item.transpose(1, 2, 0, 3).reshape(SQUARE, LAYERS, LANES)
        for item in (radial_dx, radial_dy, around_dx, around_dy, jacobian)
    ]
    advection, pressure = step_of(rows, *metrics)
    advection = advection.reshape(COMPONENTS, OWN, NODES, NODES, LAYERS, LANES)
    pressure = pressure.reshape(OWN, NODES, NODES, LAYERS, LANES)
    return (advection.transpose(0, 1, 4, 2, 3, 5), pressure.transpose(0, 3, 1, 2, 4))


def solution(mesh):
    metric = P(None, None, None, "elem")
    return jax.shard_map(
        on_device,
        mesh=mesh,
        in_specs=(P(None, "mode", None, None, None, "elem"),) + (metric,) * 5,
        out_specs=(P(None, "mode", None, None, None, "elem"), P("mode", None, None, None, "elem")),
        check_vma=False,
    )
```

```python
import functools
import itertools
import math

import jax
import jax.numpy as jnp
import numpy as np
from jax import lax
from jax.experimental import pallas as pl
from jax.experimental.pallas import tpu as pltpu
from jax.sharding import PartitionSpec as P

MESH = pl.DeviceIdType.MESH
NODES = 7
SQUARE = NODES * NODES
LAYERS = 4
ITERS = 3
COMPONENTS = 3
PLANES = 256
MODES = 64
OWN = PLANES // MODES
ELEMS = 4
LANES = 128
CELLS = COMPONENTS * SQUARE * LAYERS
CHUNKS = -(-CELLS // LANES)
PADDED = CHUNKS * LANES
FULL = CELLS // LANES
REST = CELLS - FULL * LANES
SPARE = LANES - REST
TAIL = REST - SPARE
LARGE = FULL * OWN + 3
SMALL = FULL * OWN + 2
GROUPS = PADDED // 4

spanwise_wave = 2.0 * math.pi / 64.0
time_step = 0.1

VMEM = pltpu.VMEM
DMA = pltpu.SemaphoreType.DMA


def lobatto_rule(count):
    degree = count - 1
    points = np.cos(np.pi * np.arange(count) / degree)
    legendre = np.zeros((count, count))
    for sweep in range(60):
        legendre[:, 0] = 1.0
        legendre[:, 1] = points
        for order in range(2, count):
            legendre[:, order] = (
                (2 * order - 1) * points * legendre[:, order - 1]
                - (order - 1) * legendre[:, order - 2]
            ) / order
        points = points - (points * legendre[:, degree] - legendre[:, degree - 1]) / (
            count * legendre[:, degree]
        )
    legendre[:, 0] = 1.0
    legendre[:, 1] = points
    for order in range(2, count):
        legendre[:, order] = (
            (2 * order - 1) * points * legendre[:, order - 1] - (order - 1) * legendre[:, order - 2]
        ) / order
    weights = 2.0 / (degree * count * legendre[:, degree] ** 2)
    return (points[::-1].copy(), weights[::-1].copy())


def derivative_table():
    lobatto_nodes = lobatto_rule(NODES)[0]
    total = lobatto_nodes.shape[0]
    scales = np.ones(total)
    for column in range(total):
        for other in range(total):
            if other != column:
                scales[column] = scales[column] / (lobatto_nodes[column] - lobatto_nodes[other])
    table = np.zeros((total, total))
    for row in range(total):
        for column in range(total):
            if row != column:
                table[row, column] = (
                    scales[column] / scales[row] / (lobatto_nodes[row] - lobatto_nodes[column])
                )
        table[row, row] = -np.sum(table[row])
    return table


TABLE = derivative_table().astype(np.float32)
WEIGHTS = lobatto_rule(NODES)[1]


def split(value):
    high = value.astype(jnp.bfloat16)
    return (high, (value - high.astype(jnp.float32)).astype(jnp.bfloat16))


def constant_split(value):
    value = value.astype(np.float32)
    high = value.astype(jnp.bfloat16)
    return (high, (value - high.astype(np.float32)).astype(jnp.bfloat16))


def transform_tables():
    position = np.arange(PLANES)
    plane = np.arange(PLANES)
    order = plane // 2
    angle = 2.0 * np.pi / PLANES * ((position[:, None] * order[None, :]) % PLANES)
    is_sine = (plane % 2 == 1)[None, :]
    is_top = (plane == 1)[None, :]
    parity = np.cos(np.pi * (position % 2))[:, None]
    basis = np.where(is_top, parity, np.where(is_sine, np.sin(angle), np.cos(angle)))
    scaling = np.where(order == 0, 1.0, 2.0) / PLANES
    inverse = (basis * scaling[None, :]).T
    wave = (order * spanwise_wave)[None, :]
    slope = np.where(is_sine, wave * np.cos(angle), -wave * np.sin(angle))
    forward = np.concatenate([basis.T, slope.T], axis=1)
    forward = forward.reshape(MODES, OWN, 2 * PLANES).transpose(1, 0, 2).reshape(PLANES, 2 * PLANES)
    turned = inverse.reshape(MODES, OWN, PLANES).transpose(1, 0, 2).reshape(PLANES, PLANES)
    return (*constant_split(forward), *constant_split(turned))


def contract(matrix, field):
    last, half = (NODES - 1, NODES // 2)
    even = [field[j] + field[last - j] for j in range(half)]
    odd = [field[j] - field[last - j] for j in range(half)]

    def total(terms):
        return functools.reduce(lambda x, y: x + y, terms)

    out = [None] * NODES
    for i in range(half):
        minus = [0.5 * (float(matrix[i, j]) - float(matrix[i, last - j])) for j in range(half)]
        plus = [0.5 * (float(matrix[i, j]) + float(matrix[i, last - j])) for j in range(half)]
        p = total([minus[j] * odd[j] for j in range(half)])
        q = total([plus[j] * even[j] for j in range(half)] + [float(matrix[i, half]) * field[half]])
        out[i], out[last - i] = (p + q, p - q)
    out[half] = total([float(matrix[half, j]) * odd[j] for j in range(half)])
    return out


def swap_halves(value):
    return pltpu.roll(value, 4, value.ndim - 2)


def halves(first, second):
    lower = lax.broadcasted_iota(jnp.int32, first.shape, first.ndim - 2) < 4
    return (
        jnp.where(lower, first, swap_halves(second)),
        jnp.where(lower, swap_halves(first), second),
    )


def partner(me, step):
    z, y, x = (me // 8, lax.rem(me // 2, 4), lax.rem(me, 2))
    turn_z, rest = (step // 8, 7 - lax.rem(step, 8))
    dz = 4 + turn_z // 2 - lax.rem(turn_z, 2) * (turn_z // 2 + (turn_z + 1) // 2)
    dy, dx = (rest // 2, lax.rem(rest, 2))
    return lax.rem(z + dz, 8) * 8 + lax.rem(y + dy, 4) * 2 + lax.rem(x + dx, 2)


def three_pass(first, second, dims):
    (a, b), (c, d) = (first, second)
    dot = functools.partial(
        lax.dot_general,
        dimension_numbers=(dims, ((), ())),
        preferred_element_type=jnp.float32,
    )
    return dot(a, c) + (dot(a, d) + dot(b, c))


def rows_of(ref):
    return ref.reshape(MODES * ref.shape[1], LANES)


def put(ref, row, value):
    rows_of(ref)[pl.ds(row, MODES, stride=ref.shape[1]), :] = value


def take(ref, row):
    return rows_of(ref)[pl.ds(row, MODES, stride=ref.shape[1]), :]


def before(bound, first, second):
    lane = lax.broadcasted_iota(jnp.int32, first.shape, 1)
    return jnp.where(lane < bound, first, second)


def turn(value, amount):
    return pltpu.roll(value, amount % LANES, 1)


def put_large(ref, x, small_rest):
    put(ref, FULL * OWN, before(REST, x[0], turn(x[3], REST)))
    put(ref, FULL * OWN + 1, before(REST, x[1], turn(x[3], TAIL)))
    rest = before(REST + TAIL, turn(small_rest[0], TAIL), turn(small_rest[1], 2 * TAIL))
    put(ref, FULL * OWN + 2, before(REST, x[2], rest))


def put_small(ref, y):
    put(ref, FULL * OWN, before(REST, y[0], turn(y[3], REST)))
    put(ref, FULL * OWN + 1, before(REST, y[1], turn(y[2], REST)))


def take_large(ref):
    x = [take(ref, FULL * OWN + i) for i in range(3)]
    return x + [before(SPARE, turn(x[0], -REST), turn(x[1], -TAIL))]


def take_small(ref, large):
    y = [take(ref, FULL * OWN + i) for i in range(2)]
    rest = take(large, FULL * OWN + 2)
    return y + [
        before(SPARE, turn(y[1], -REST), turn(rest, -TAIL)),
        before(SPARE, turn(y[0], -REST), turn(rest, -2 * TAIL)),
    ]


def send_all(source, target, send_sem, receive_sem, me):
    def one(step, carry):
        other = partner(me, step)
        pltpu.make_async_remote_copy(
            src_ref=source.at[other],
            dst_ref=target.at[me],
            send_sem=send_sem,
            recv_sem=receive_sem,
            device_id={"mode": other},
            device_id_type=MESH,
        ).start()
        return carry

    lax.fori_loop(0, MODES - 1, one, 0)
    target[me] = source[me]


def wait_all(buffer, sem):
    others = buffer.at[pl.ds(0, MODES - 1)]
    pltpu.make_async_copy(others, others, sem).wait()


def step_kernel(velocity, radial_dx, radial_dy, around_dx, around_dy, jacobian,
                forward_high, forward_low, back_high, back_low, advection, out,
                rows, posted_0, posted_1, got_0, got_1, answer_0, answer_1, returned_0, returned_1, local, values, result, predicted,
                fields, edges, geometry, tables, metrics, stiff, residual, direction, carried,
                image_raw, radial_s, around_s, rims, posts,
                load_sem, send_sem, receive_sem, rim_send_sem, rim_receive_sem):
    loads = [pltpu.make_async_copy(velocity, fields, load_sem.at[0])]
    for i, metric in enumerate((radial_dx, radial_dy, around_dx, around_dy, jacobian)):
        loads.append(pltpu.make_async_copy(metric, geometry.at[i], load_sem.at[1 + i]))
    for i, table in enumerate((forward_high, forward_low)):
        loads.append(pltpu.make_async_copy(table, tables.at[i], load_sem.at[6 + i]))
    for i, table in enumerate((back_high, back_low)):
        loads.append(pltpu.make_async_copy(table, edges.at[i], load_sem.at[8 + i]))
    loads[0].start()
    me = lax.axis_index("mode")
    barrier = pltpu.get_barrier_semaphore()

    def greet(step, carry):
        pl.semaphore_signal(
            barrier, inc=1, device_id={"mode": partner(me, step)}, device_id_type=MESH
        )
        return carry

    lax.fori_loop(0, MODES - 1, greet, 0)
    here = lax.axis_index("elem")
    for step in range(1, ELEMS):
        pl.semaphore_signal(
            barrier, inc=1, device_id={"elem": lax.rem(here + step, ELEMS)}, device_id_type=MESH
        )
    loads[0].wait()
    for load in loads[1:]:
        load.start()

    posted, got = ((posted_0, posted_1), (got_0, got_1))
    answer, returned = ((answer_0, answer_1), (returned_0, returned_1))
    last = ([], [])
    for p in range(OWN):
        for c in range(COMPONENTS):
            start = (c * OWN + p) * SQUARE * LAYERS
            rows[p, pl.ds(c * SQUARE * LAYERS, SQUARE * LAYERS), :] = fields[
                pl.ds(start, SQUARE * LAYERS), :
            ]
        rows[p, pl.ds(CELLS, PADDED - CELLS), :] = jnp.zeros((PADDED - CELLS, LANES), jnp.float32)
        for k in range(CHUNKS):
            turned = rows[p, pl.ds(k * LANES, LANES), :].T
            for t in range(2):
                part = turned[t * MODES : (t + 1) * MODES]
                if k < FULL:
                    put(posted[t], k * OWN + p, part)
                else:
                    last[t].append(part)
    put_large(posted_0, last[0], last[1][2:])
    put_small(posted_1, last[1])
    pl.semaphore_wait(barrier, MODES - 1 + ELEMS - 1)
    for t in range(2):
        send_all(posted[t], got[t], send_sem.at[0, t], receive_sem.at[0, t], me)

    for load in loads[1:]:
        load.wait()
    lane = lax.broadcasted_iota(jnp.int32, (SQUARE, LAYERS, LANES), 2)
    for t in range(2):
        for i in range(4):
            chosen = jnp.where(lane == me + t * MODES, geometry[i], 0.0)
            picked = jnp.sum(chosen, axis=2, keepdims=True)
            local[t, i] = jnp.broadcast_to(-picked, (SQUARE, LAYERS, LANES))

    sub = lax.broadcasted_iota(jnp.int32, (8, LANES), 0)
    lane = lax.broadcasted_iota(jnp.int32, (8, LANES), 1)
    layer = lax.rem(sub, 4)
    even = sub < 4
    inside = layer < LAYERS - 1
    above = layer > 0
    pairs = range(OWN // 2)
    nodes = range(NODES)

    for i in range(5):
        metrics[i] = jnp.concatenate([geometry[i]] * 2, axis=1)

    for a in nodes:
        for b in nodes:
            node = a * NODES + b
            rx, ry, ax, ay, jac = (metrics[i, node] for i in range(5))
            mass = float(np.float32(WEIGHTS[a] * WEIGHTS[b])) * jac
            stiff[0, a, b] = mass * (rx * rx + ry * ry)
            stiff[1, a, b] = mass * (rx * ax + ry * ay)
            stiff[2, a, b] = mass * (ax * ax + ay * ay)
            stiff[3, a, b] = mass

    zero = jnp.zeros((LAYERS, PLANES), jnp.float32)
    for g in range(COMPONENTS * SQUARE, GROUPS):
        result[g] = zero
    small_rest = []
    for t in range(2):
        wait_all(got[t], receive_sem.at[0, t])
        rest = take_small(got_1, got_0) if t else take_large(got_0)
        planes = jnp.concatenate(
            [
                jnp.concatenate([take(got[t], k * OWN + p) for p in range(OWN)], axis=0)
                for k in range(FULL)
            ]
            + [jnp.concatenate(rest, axis=0)],
            axis=1,
        )
        physical = three_pass(split(planes), (tables[0], tables[1]), ((0,), (0,)))
        values[...] = physical.reshape(GROUPS, LAYERS, 2 * PLANES)
        for a in range(NODES):
            for b in range(NODES):
                node = a * NODES + b
                mx, my, nx, ny = (
                    jnp.concatenate([local[t, i, node]] * 2, axis=1) for i in range(4)
                )
                u = values[node, :, :PLANES]
                v = values[SQUARE + node, :, :PLANES]
                w = values[2 * SQUARE + node, :, :PLANES]
                along = u * mx + v * my
                across = u * nx + v * ny
                for c in range(COMPONENTS):
                    radial, beside = (zero, zero)
                    for i in range(NODES):
                        radial += float(TABLE[a, i]) * values[c * SQUARE + i * NODES + b, :, :PLANES]
                        beside += float(TABLE[b, i]) * values[c * SQUARE + a * NODES + i, :, :PLANES]
                    slope = values[c * SQUARE + node, :, PLANES:]
                    result[c * SQUARE + node] = radial * along + beside * across - slope * w
        spectral = three_pass(
            (edges[0], edges[1]),
            split(result[...].reshape(PADDED, PLANES)),
            ((1,), (1,)),
        )
        last = []
        for p in range(OWN):
            part = spectral[p * MODES : (p + 1) * MODES]
            for k in range(FULL):
                put(answer[t], k * OWN + p, part[:, k * LANES : (k + 1) * LANES])
            last.append(part[:, FULL * LANES :])
        if t:
            put_large(answer_1, last, small_rest)
        else:
            put_small(answer_0, last)
            small_rest = last[2:]
        send_all(answer[t], returned[t], send_sem.at[1, t], receive_sem.at[1, t], me)
    for t in range(2):
        wait_all(returned[t], receive_sem.at[1, t])

    rest = (take_small(returned_0, returned_1), take_large(returned_1))
    for p in range(OWN):
        for k in range(CHUNKS):
            block = jnp.concatenate(
                [
                    take(returned[t], k * OWN + p) if k < FULL else rest[t][p]
                    for t in range(2)
                ],
                axis=0,
            )
            rows[p, pl.ds(k * LANES, LANES), :] = block.T
        for c in range(COMPONENTS):
            there = pl.ds((c * OWN + p) * SQUARE * LAYERS, SQUARE * LAYERS)
            own = pl.ds(c * SQUARE * LAYERS, SQUARE * LAYERS)
            term = rows[p, own, :]
            rows[p, own, :] = fields[there, :] + time_step * term
            advection[there, :] = term
    for pair in range(OWN // 2):
        first, second = halves(
            rows[2 * pair].reshape(PADDED // 8, 8, LANES),
            rows[2 * pair + 1].reshape(PADDED // 8, 8, LANES),
        )
        for q in range(PADDED // 8):
            predicted[pair, 2 * q] = first[q]
            predicted[pair, 2 * q + 1] = second[q]

    orders = [(me * (OWN // 2) + pair).astype(jnp.float32) for pair in pairs]
    waves = [jnp.full((8, LANES), order) * spanwise_wave for order in orders]
    tops = [
        jnp.where((jnp.full((8, LANES), order) == 0.0) & (sub >= 4), float(PLANES // 2), order)
        * spanwise_wave
        for order in orders
    ]
    shifts = [top * top for top in tops]

    def right_side(pair):
        wave = jnp.where(even, waves[pair], -waves[pair])
        for b in nodes:
            for c, kept in enumerate((radial_s, around_s)):
                radial = contract(
                    TABLE, [predicted[pair, c * SQUARE + a * NODES + b] for a in nodes]
                )
                for a in nodes:
                    kept[a, b] = radial[a]
        for a in nodes:
            beside = [
                contract(TABLE, [predicted[pair, c * SQUARE + a * NODES + b] for b in nodes])
                for c in range(2)
            ]
            for b in nodes:
                node = a * NODES + b
                rx, ry, ax, ay = (metrics[i, node] for i in range(4))
                divergence = (
                    (rx * radial_s[a, b] + ax * beside[0][b])
                    + (ry * around_s[a, b] + ay * beside[1][b])
                    + wave * swap_halves(predicted[pair, 2 * SQUARE + node])
                )
                image_raw[pair, a, b] = (stiff[3, a, b] * divergence) * (-1.0 / time_step)

    def across_layers(pair):
        low = [image_raw[pair, 0, b] for b in nodes]
        high = [image_raw[pair, NODES - 1, b] for b in nodes]
        for b in nodes:
            other, this = (pltpu.roll(high[b], 1, 0), pltpu.roll(low[b], 7, 0))
            image_raw[pair, 0, b] = low[b] + jnp.where(above, other, 0.0)
            image_raw[pair, NODES - 1, b] = jnp.where(inside, high[b] + this, 0.0)

    def post(phase, pair, dots):
        first = jnp.zeros((8, LANES), jnp.float32)
        if phase < ITERS:
            for a in nodes:
                start = image_raw[pair, a, 0]
                end = image_raw[pair, a, NODES - 1]
                first = jnp.where(lane == a, pltpu.roll(start, a, 1) if a else start, first)
                first = jnp.where(lane == 32 + a, pltpu.roll(end, 33 + a, 1), first)
        for index, dot in enumerate(dots):
            total = jnp.sum(dot, axis=1, keepdims=True)
            first = jnp.where(lane == 8 + index, total, first)
        posts[phase, pair] = first
        rims[phase, pair, here] = first
        copies = []
        for step in range(1, ELEMS):
            copy = pltpu.make_async_remote_copy(
                src_ref=posts.at[phase, pair],
                dst_ref=rims.at[phase, pair, here],
                send_sem=rim_send_sem.at[phase, pair, step],
                recv_sem=rim_receive_sem.at[phase, pair, step],
                device_id={"elem": lax.rem(here + step, ELEMS)},
                device_id_type=MESH,
            )
            copy.start()
            copies.append(copy)
        return copies

    def collect(phase, pair, copies, count):
        for copy in copies:
            copy.wait()
        came = [rims[phase, pair, i] for i in range(ELEMS)]
        total = (came[0] + came[1]) + (came[2] + came[3])
        sums = []
        for index in range(count):
            column = jnp.sum(jnp.where(lane == 8 + index, total, 0.0), axis=1, keepdims=True)
            column = jnp.broadcast_to(column, (8, LANES))
            lower = jnp.sum(jnp.where(even, column, 0.0), axis=0, keepdims=True)
            upper = jnp.sum(jnp.where(even, 0.0, column), axis=0, keepdims=True)
            sums.append(jnp.where(even, lower, upper))
        right = rims[phase, pair, lax.rem(here + 1, ELEMS)]
        left = rims[phase, pair, lax.rem(here + ELEMS - 1, ELEMS)]
        return (sums, left, right)

    def across_columns(pair, a, left, right):
        slot = a
        start = image_raw[pair, a, 0]
        end = image_raw[pair, a, NODES - 1]
        after = jnp.where(
            lane == LANES - 1, pltpu.roll(right, LANES - 1 - slot, 1), pltpu.roll(start, LANES - 1, 1)
        )
        before = jnp.where(lane == 0, pltpu.roll(left, LANES - 32 - slot, 1), pltpu.roll(end, 1, 1))
        return (start + before, end + after)

    weight_a = [
        jnp.where(above, 0.5, 1.0) if a == 0 else jnp.where(inside, 0.5, 0.0) if a == NODES - 1 else None
        for a in nodes
    ]

    gamma_old = [None, None]
    inner_old = [None, None]
    def apply(pair):
        for b in nodes:
            radial = contract(TABLE, [residual[pair, a, b] for a in nodes])
            for a in nodes:
                radial_s[a, b] = radial[a]
        norm = jnp.zeros((8, LANES), jnp.float32)
        for a in nodes:
            slab = [residual[pair, a, b] for b in nodes]
            beside = contract(TABLE, slab)
            spread = []
            for b in nodes:
                g11, g12, g22 = (stiff[i, a, b] for i in range(3))
                radial = radial_s[a, b]
                radial_s[a, b] = g11 * radial + g12 * beside[b]
                spread.append(g12 * radial + g22 * beside[b])
            spread = contract(TABLE.T, spread)
            squares = [item * item for item in slab]
            row = 0.5 * (squares[0] + squares[NODES - 1])
            for b in nodes:
                image_raw[pair, a, b] = spread[b] + shifts[pair] * stiff[3, a, b] * slab[b]
                if 0 < b < NODES - 1:
                    row = row + squares[b]
            norm = norm + (row if weight_a[a] is None else row * weight_a[a])
        product = jnp.zeros((8, LANES), jnp.float32)
        for b in nodes:
            radial = contract(TABLE.T, [radial_s[a, b] for a in nodes])
            for a in nodes:
                value = image_raw[pair, a, b] + radial[a]
                image_raw[pair, a, b] = value
                product = product + residual[pair, a, b] * value
        return [norm, product]

    def update(turn, pair, sums, left, right):
        gamma, delta = sums
        if turn == 0:
            beta, inner = (None, delta)
        else:
            beta = gamma / gamma_old[pair]
            inner = delta - beta * beta * inner_old[pair]
        alpha = gamma / inner
        gamma_old[pair], inner_old[pair] = (gamma, inner)
        for a in nodes:
            if turn < ITERS - 1:
                start, end = across_columns(pair, a, left, right)
            for b in nodes:
                now = residual[pair, a, b]
                if turn:
                    now = now + beta * direction[pair, a, b]
                step = alpha * now
                total = step if turn == 0 else predicted[pair, a * NODES + b] + step
                if turn == ITERS - 1:
                    for h in range(2):
                        out[2 * pair + h, a * NODES + b] = total[h * LAYERS : (h + 1) * LAYERS]
                else:
                    predicted[pair, a * NODES + b] = total
                if turn < ITERS - 1:
                    direction[pair, a, b] = now
                    image = start if b == 0 else end if b == NODES - 1 else image_raw[pair, a, b]
                    if turn:
                        image = image + beta * carried[pair, a, b]
                    carried[pair, a, b] = image
                    residual[pair, a, b] = residual[pair, a, b] - alpha * image

    copies = [None, None]
    for pair in pairs:
        right_side(pair)
        across_layers(pair)
        copies[pair] = post(0, pair, [])
    for phase in range(ITERS + 1):
        for pair in pairs:
            sums, left, right = collect(phase, pair, copies[pair], 2 if phase else 0)
            if phase:
                update(phase - 1, pair, sums, left, right)
            else:
                for a in nodes:
                    start, end = across_columns(pair, a, left, right)
                    for b in nodes:
                        raw = image_raw[pair, a, b]
                        residual[pair, a, b] = start if b == 0 else end if b == NODES - 1 else raw
            if phase < ITERS:
                dots = apply(pair)
                if phase < ITERS - 1:
                    across_layers(pair)
                copies[pair] = post(phase + 1, pair, dots)

    for t in range(2):
        wait_all(posted[t], send_sem.at[0, t])
        wait_all(answer[t], send_sem.at[1, t])


def step_of(velocity, *metrics):
    tables = transform_tables()
    large, small = (VMEM((MODES, rows, 1, LANES), jnp.float32) for rows in (LARGE, SMALL))
    field = VMEM((OWN // 2, NODES, NODES, 8, LANES), jnp.float32)
    slabs = VMEM((NODES, NODES, 8, LANES), jnp.float32)
    return pl.pallas_call(
        step_kernel,
        out_shape=(
            jax.ShapeDtypeStruct(velocity.shape, jnp.float32),
            jax.ShapeDtypeStruct((OWN, SQUARE, LAYERS, LANES), jnp.float32),
        ),
        in_specs=[pl.BlockSpec(memory_space=pltpu.HBM)] * 10,
        out_specs=(pl.BlockSpec(memory_space=VMEM),) * 2,
        scratch_shapes=[
            VMEM((OWN, PADDED, LANES), jnp.float32),
            large,
            small,
            large,
            small,
            small,
            large,
            small,
            large,
            VMEM((2, 4, SQUARE, LAYERS, LANES), jnp.float32),
            VMEM((GROUPS, LAYERS, 2 * PLANES), jnp.float32),
            VMEM((GROUPS, LAYERS, PLANES), jnp.float32),
            VMEM((OWN // 2, GROUPS, 8, LANES), jnp.float32),
            VMEM(velocity.shape, jnp.float32),
            VMEM((2, PLANES, PLANES), jnp.bfloat16),
            VMEM((5, SQUARE, LAYERS, LANES), jnp.float32),
            VMEM((2, PLANES, 2 * PLANES), jnp.bfloat16),
            VMEM((5, SQUARE, 8, LANES), jnp.float32),
            VMEM((4, NODES, NODES, 8, LANES), jnp.float32),
            field,
            field,
            field,
            field,
            slabs,
            slabs,
            VMEM((ITERS + 1, OWN // 2, ELEMS, 8, LANES), jnp.float32),
            VMEM((ITERS + 1, OWN // 2, 8, LANES), jnp.float32),
            DMA((10,)),
            DMA((2, 2)),
            DMA((2, 2)),
            DMA((ITERS + 1, OWN // 2, ELEMS)),
            DMA((ITERS + 1, OWN // 2, ELEMS)),
        ],
        compiler_params=pltpu.CompilerParams(
            collective_id=1, has_side_effects=True, vmem_limit_bytes=40 << 20
        ),
        name="step",
    )(
        *(
            pltpu.with_memory_space_constraint(item, pltpu.HBM)
            for item in (velocity, *metrics, *(jnp.asarray(t) for t in tables))
        )
    )


def on_device(velocity, radial_dx, radial_dy, around_dx, around_dy, jacobian):
    rows = velocity.transpose(0, 1, 3, 4, 2, 5).reshape(COMPONENTS * OWN * SQUARE * LAYERS, LANES)
    metrics = [
        item.transpose(1, 2, 0, 3).reshape(SQUARE, LAYERS, LANES)
        for item in (radial_dx, radial_dy, around_dx, around_dy, jacobian)
    ]
    advection, pressure = step_of(rows, *metrics)
    advection = advection.reshape(COMPONENTS, OWN, NODES, NODES, LAYERS, LANES)
    pressure = pressure.reshape(OWN, NODES, NODES, LAYERS, LANES)
    return (advection.transpose(0, 1, 4, 2, 3, 5), pressure.transpose(0, 3, 1, 2, 4))


def solution(mesh):
    metric = P(None, None, None, "elem")
    return jax.shard_map(
        on_device,
        mesh=mesh,
        in_specs=(P(None, "mode", None, None, None, "elem"),) + (metric,) * 5,
        out_specs=(P(None, "mode", None, None, None, "elem"), P("mode", None, None, None, "elem")),
        check_vma=False,
    )
```
